128 devices in a mesh: head: 4 (over y_hi, core), seq: 32 (over x, z, y_lo).
Axes of the slice: x: 4, y: 4 (y_hi: 2, y_lo: 2; y = y_hi * 2 + y_lo), z: 4, core: 2. Of those that a mesh axis runs over, the one named last changes fastest.
Arguments:
- queries: bfloat16 [32768, 4096], P('seq', 'head'), may hold values from -6 to 6
- keys: bfloat16 [32768, 512], P('seq', 'head'), may hold values from -6 to 6
- values: bfloat16 [32768, 512], P('seq', 'head'), may hold values from -6 to 6
- vertical: int32 [32, 8], P('head'), may hold values from 0 to 255, as said below
- slash: int32 [32, 8], P('head'), may hold values from 1 to 28, as said below
Outputs:
- attended: bfloat16 [32768, 4096], P(('seq', 'head'))
The draws below stay inside these ranges and needn't reach their ends.
Inputs may be any that keep to these rules, and one draw needn't show every extreme that they name: `vertical`: each row names 8 different blocks. Within each group of 8 consecutive rows, the different blocks named that lie in one slab (blocks s * 8 to s * 8 + 7) number at most 4, and exactly 4 in some slab. `slash`: each row names 8 different offsets.
All inputs are finite; a program needn't handle non-finite values.
Results may differ from the reference program's by a relative error of at most 0.0033.
Values may be sent and summed in bfloat16 or wider, within the bound.
A program may use at most 128 MiB of HBM per device.

```python
import math
import jax
import jax.numpy as jnp
from jax import lax

HD = 128
QUERY_PER_GROUP = 8
BLK = 128
VERTICAL_BLOCKS = 8
SLASH_OFFSETS = 8
LARGEST_OFFSET = 28
CAP = 4
GROUPS = 4
HEADS = 32
BLK_DEV = 8
SLABS = 32
SEQ = 32768
BLOCKS = 256


def draw_queries(key, part):
    own_key = jax.random.fold_in(key, 11)
    drawn = jnp.clip(1.5 * jax.random.normal(own_key, (SEQ, GROUPS, QUERY_PER_GROUP, HD), jnp.float32), -6.0, 6.0)
    return drawn.reshape(SEQ, HEADS * HD).astype(jnp.bfloat16)


def draw_keys(key, part):
    own_key = jax.random.fold_in(key, 12)
    drawn = jnp.clip(1.5 * jax.random.normal(own_key, (SEQ, GROUPS, HD), jnp.float32), -6.0, 6.0)
    return drawn.reshape(SEQ, GROUPS * HD).astype(jnp.bfloat16)


def vertical_group(key):
    key_count, key_full, key_order, key_pick = jax.random.split(key, 4)
    slab_ids = jnp.arange(SLABS, dtype=jnp.int32)
    counts = jax.random.randint(key_count, (SLABS,), 1, CAP + 1)
    fullest = jax.random.randint(key_full, (), 0, SLABS)
    counts = jnp.where(slab_ids == fullest, CAP, counts)
    order_scores = jax.random.randint(key_order, (SLABS, BLK_DEV), 0, 4096) * BLK_DEV + jnp.arange(BLK_DEV, dtype=jnp.int32)[None, :]
    ranks = jnp.argsort(jnp.argsort(order_scores, axis=1), axis=1)
    inside = ranks < counts[:, None]
    mandatory_blocks = (inside & (slab_ids[:, None] == fullest)).reshape(BLOCKS)
    inside = inside.reshape(BLOCKS)
    selected_indices = jax.random.randint(key_pick, (QUERY_PER_GROUP, BLOCKS), 0, 65536) * BLOCKS + jnp.arange(BLOCKS, dtype=jnp.int32)[None, :] + 1
    selected_indices = jnp.where(inside[None, :], selected_indices, 0)
    extra_score = jnp.where((jnp.arange(QUERY_PER_GROUP)[:, None] == 0) & mandatory_blocks[None, :], 1 << 29, 0)
    leftover_slots, selected_blocks = lax.top_k(selected_indices + extra_score, VERTICAL_BLOCKS)
    return selected_blocks.astype(jnp.int32)


def draw_vertical(key, part):
    group_keys = jax.random.split(jax.random.fold_in(key, 31), GROUPS)
    return jax.vmap(vertical_group)(group_keys).reshape(HEADS, VERTICAL_BLOCKS).astype(jnp.int32)


def draw_slash(key, part):
    block_scores = jax.random.randint(jax.random.fold_in(key, 41), (HEADS, LARGEST_OFFSET), 0, 65536) * LARGEST_OFFSET + jnp.arange(LARGEST_OFFSET, dtype=jnp.int32)[None, :] + 1
    per_head_rows = jnp.arange(HEADS)[:, None]
    offset_columns = jnp.arange(LARGEST_OFFSET)[None, :]
    extra_score = jnp.where((per_head_rows == 0) & (offset_columns == LARGEST_OFFSET - 1), 1 << 28, 0)
    extra_score = extra_score + jnp.where((per_head_rows == 1) & (offset_columns == 0), 1 << 28, 0)
    leftover_slots, selected_blocks = lax.top_k(block_scores + extra_score, SLASH_OFFSETS)
    return (selected_blocks + 1).astype(jnp.int32)


def block_levels(key, extent, pieces, least, largest):
    factor_of, own = 1.0, jax.random.fold_in(key, 6)
    for position, shards_of in pieces:
        steps = jnp.exp(jax.random.uniform(jax.random.fold_in(own, position), (shards_of,), jnp.float32, least / len(pieces), largest / len(pieces)))
        factor_of = factor_of * jnp.repeat(steps, extent[position] // shards_of).reshape([-1 if axis == position else 1 for axis in range(len(extent))])
    return factor_of


def normal_values(rng, dims, scale, limit, cuts=(), held_as=jnp.bfloat16):
    level = block_levels(rng, dims, cuts, -0.22, 0.18) if cuts else 1.0
    values = jax.random.normal(rng, dims, jnp.float32) * scale * level
    return jnp.minimum(jnp.maximum(values, -limit), limit).astype(held_as)


def setup_inputs(seed: int = 0) -> dict:
    key_list = jax.random.split(jax.random.key(seed), 6)
    return {
        "queries": draw_queries(jax.random.fold_in(key_list[5], 71), 0),
        "keys": draw_keys(jax.random.fold_in(key_list[5], 71), 0),
        "values": normal_values(key_list[2], (SEQ, GROUPS * HD), 1.0, 6.0, ((0, 32), (1, 4))),
        "vertical": draw_vertical(jax.random.fold_in(key_list[5], 71), 0),
        "slash": draw_slash(jax.random.fold_in(key_list[5], 71), 0),
    }


NEG = -1e+30

def attend(query_block, diag_kv, slash_kv, column_kv, slash_ok, column_ok):
    block_count, block_width, head_width = query_block.shape
    slash_count = slash_kv.shape[1]
    column_count = column_kv.shape[0]
    score_scale = 1.0 / math.sqrt(head_width)
    causal = jnp.arange(block_width)[:, None] >= jnp.arange(block_width)[None, :]
    diag_scores = jnp.einsum('ird,icd->irc', query_block, diag_kv[..., :head_width]) * score_scale
    diag_scores = jnp.where(causal[None], diag_scores, NEG)
    slash_scores = jnp.einsum('ird,ijcd->irjc', query_block, slash_kv[..., :head_width]) * score_scale
    slash_scores = jnp.where(slash_ok[:, None, :, None], slash_scores, NEG).reshape(block_count, block_width, slash_count * block_width)
    column_scores = jnp.einsum('ird,jcd->irjc', query_block, column_kv[..., :head_width]) * score_scale
    column_scores = jnp.where(column_ok[:, None, :, None], column_scores, NEG).reshape(block_count, block_width, column_count * block_width)
    block_scores = jnp.concatenate([diag_scores, slash_scores, column_scores], axis=2)
    row_top = lax.optimization_barrier(jnp.max(block_scores, axis=2, keepdims=True))
    weights = jnp.exp(block_scores - row_top)
    row_total = lax.optimization_barrier(jnp.sum(weights, axis=2))
    rounded = lax.optimization_barrier(weights.astype(jnp.bfloat16)).astype(jnp.float32)
    split_one = block_width
    split_two = block_width + slash_count * block_width
    w_diag = rounded[:, :, :split_one]
    w_slash = rounded[:, :, split_one:split_two].reshape(block_count, block_width, slash_count, block_width)
    w_column = rounded[:, :, split_two:].reshape(block_count, block_width, column_count, block_width)
    mixed_sum = jnp.einsum('irc,icd->ird', w_diag, diag_kv[..., head_width:])
    mixed_sum = mixed_sum + jnp.einsum('irjc,ijcd->ird', w_slash, slash_kv[..., head_width:])
    mixed_sum = mixed_sum + jnp.einsum('irjc,jcd->ird', w_column, column_kv[..., head_width:])
    return (mixed_sum / row_total[:, :, None]).astype(jnp.bfloat16)

def reference(queries, keys, values, vertical, slash):
    seq_rows = queries.shape[0]
    block_total = seq_rows // BLK
    joined = jnp.concatenate([keys.reshape(seq_rows, GROUPS, HD), values.reshape(seq_rows, GROUPS, HD)], axis=2)
    block_ids = jnp.arange(block_total, dtype=jnp.int32)

    def one_head(head_index):
        group_index = head_index // QUERY_PER_GROUP
        query_block = lax.dynamic_slice_in_dim(queries, head_index * HD, HD, 1).astype(jnp.float32).reshape(block_total, BLK, HD)
        group_kv = lax.dynamic_index_in_dim(joined, group_index, 1, keepdims=False).astype(jnp.float32).reshape(block_total, BLK, 2 * HD)
        padded = jnp.concatenate([jnp.zeros((LARGEST_OFFSET, BLK, 2 * HD), jnp.float32), group_kv], axis=0)
        offsets = lax.dynamic_index_in_dim(slash, head_index, 0, keepdims=False)
        columns = lax.dynamic_index_in_dim(vertical, head_index, 0, keepdims=False)
        slash_index = (LARGEST_OFFSET + block_ids[:, None] - offsets[None, :]).astype(jnp.int32)
        slash_kv = jnp.take(padded, slash_index, axis=0)
        slash_ok = block_ids[:, None] - offsets[None, :] >= 0
        column_kv = jnp.take(group_kv, columns.astype(jnp.int32), axis=0)
        covered = jnp.any(block_ids[:, None, None] - columns[None, :, None] == offsets[None, None, :], axis=2)
        column_ok = (columns[None, :] < block_ids[:, None]) & jnp.logical_not(covered)
        return attend(query_block, group_kv, slash_kv, column_kv, slash_ok, column_ok)
    outputs = lax.map(one_head, jnp.arange(HEADS, dtype=jnp.int32))
    return jnp.transpose(outputs, (1, 2, 0, 3)).reshape(seq_rows, HEADS * HD)
```

```python
import functools
import math

import jax
import jax.numpy as jnp
from jax import lax
from jax.experimental import pallas as pl
from jax.experimental.pallas import tpu as pltpu
from jax.sharding import PartitionSpec as P

BLK = 128
LARGEST_OFFSET = 28
CAP = 4
NEG = -1e30
SIDE = 4
NODES = SIDE * SIDE
REACH = 4
HALF = CAP // 2
MESH = pl.DeviceIdType.MESH

COPIES = {}
COPIES["zp"] = ((0, 1), (0, 0), "full")
COPIES["zm"] = ((0, -1), (0, 0), "full")
COPIES["xp"] = ((1, 0), (0, 0), "full")
COPIES["xm"] = ((-1, 0), (0, 0), "full")
COPIES["zm2"] = ((0, -1), (0, 1), "full")
COPIES["xm2"] = ((-1, 0), (1, 0), "full")
for d in (1, -1, 2):
    COPIES["xpA", d] = ((1, 0), (0, d), "A")
    COPIES["xmA", d] = ((-1, 0), (0, d), "A")
    COPIES["xmA2", d] = ((-1, 0), (1, d), "A")
    COPIES["zpB", d] = ((0, 1), (d, 0), "B")
    COPIES["zmB", d] = ((0, -1), (d, 0), "B")
    COPIES["zmB2", d] = ((0, -1), (d, 1), "B")
NAMES = list(COPIES)

THEN = {name: [] for name in NAMES}
THEN["zm"] = ["zm2", ("xpA", 1), ("xmA", 1)]
THEN["zm2"] = [("xpA", 2), ("xmA", 2)]
THEN["zp"] = [("xpA", -1), ("xmA", -1)]
THEN["xm"] = ["xm2", ("zpB", 1), ("zmB", 1)]
THEN["xm2"] = [("zpB", 2), ("zmB", 2)]
THEN["xp"] = [("zpB", -1), ("zmB", -1)]
for d in (1, -1, 2):
    THEN["xmA", d] = [("xmA2", d)]
    THEN["zmB", d] = [("zmB2", d)]

FIRST = ["xm", "zm", "xp"]
SECOND = ["xm2", "zm2", ("zmB", 1), ("xmA", 1), ("xpA", 1)]
LATER = [
    [("zmB", -1)],
    [("xmA", 2)],
    [("zmB", 2)],
    ["zp"],
    [("xpA", 2)],
    [("zmB2", 1)],
    [("xmA2", 1)],
    [("zmB2", -1)],
    [("xmA", -1)],
    [("zpB", 1), ("xpA", -1)],
    [("zmB2", 2), ("xmA2", 2)],
    [("zpB", -1)],
    [("zpB", 2), ("xmA2", -1)],
]


def attended(slot, weights_of, blocks_of, pairs):
    mixed = None
    for n in range(pairs):
        part = jnp.dot(weights_of(n), blocks_of(n), preferred_element_type=jnp.float32)
        mixed = part if mixed is None else mixed + part
    return mixed


def layer_kernel(
    slash_ref,
    vertical_ref,
    queries_ref,
    kt_ref,
    v_ref,
    out_ref,
    table_v,
    table_s,
    found_v,
    found_s,
    q_ref,
    own_ref,
    near,
    far,
    staged,
    mixed_ref,
    top_ref,
    total_ref,
    scores_0,
    scores_1,
    scores_2,
    scores_3,
    tops,
    load_sem,
    swap_send,
    swap_recv,
    table_sem,
    near_send,
    near_recv,
    unit_send,
    unit_recv,
    twin_send,
    twin_recv,
    out_local,
    out_send,
    out_recv,
    *,
    blocks,
    heads,
    width,
    listed,
):
    seq, head = lax.axis_index("seq"), lax.axis_index("head")
    node, low = seq // 2, seq % 2
    high, core = head // 2, head % 2
    x, z = node // SIDE, node % SIDE
    group, slab = 2 * high + low, 2 * node + core
    native = low == core
    scores = (scores_0, scores_1, scores_2, scores_3)
    half = blocks // 2

    def at(dx, dz):
        to = lax.rem(x + dx + SIDE, SIDE) * SIDE + lax.rem(z + dz + SIDE, SIDE)
        return {"seq": 2 * to + low}

    follower = {"seq": 2 * lax.rem(node + 1, NODES) + low}
    leader = {"seq": 2 * lax.rem(node + NODES - 1, NODES) + low}
    twin = {"head": 2 * high + 1 - core}
    counterpart = {"seq": 2 * node + core, "head": 2 * high + low}

    def owner_of(quarter):
        return {"seq": slab, "head": quarter}

    def worker_of(of_group):
        return {"seq": 2 * node + lax.rem(of_group, 2), "head": 2 * (of_group // 2) + low}

    sources = [slash_ref, vertical_ref, kt_ref, v_ref]
    targets = [table_v.at[0], table_v.at[1], own_ref.at[:, 0], own_ref.at[:, 1]]
    for i in range(blocks):
        rows = pl.ds(i * BLK, BLK)
        sources.append(queries_ref.at[rows])
        targets.append(q_ref.at[rows])

    def load(k):
        return pltpu.make_async_copy(sources[k], targets[k], load_sem.at[k])

    def swap(k):
        return pltpu.make_async_remote_copy(
            sources[k], targets[k], swap_send.at[k], swap_recv.at[k],
            device_id=counterpart, device_id_type=MESH,
        )

    def wait_input(k):
        @pl.when(native)
        def _():
            load(k).wait()

        @pl.when(jnp.logical_not(native))
        def _():
            swap(k).wait_recv()

    @pl.when(native)
    def _():
        for k in range(len(sources)):
            load(k).start()

    barrier = pltpu.get_barrier_semaphore()

    def greet(device):
        pl.semaphore_signal(barrier, 1, device_id=device, device_id_type=MESH)

    for device in (at(1, 0), at(-1, 0), at(0, 1), at(0, -1), follower, leader, twin):
        greet(device)
    for k in range(4):

        @pl.when(jnp.logical_not(native & (head == k)))
        def _():
            greet(owner_of(k))

        @pl.when(jnp.logical_not(native & (group == k)))
        def _():
            greet(worker_of(jnp.int32(k)))

    @pl.when(jnp.logical_not(native))
    def _():
        greet(counterpart)

    pl.semaphore_wait(barrier, 7 + 6 + 3 * (low - core) * (low - core))

    @pl.when(jnp.logical_not(native))
    def _():
        for k in range(len(sources)):
            swap(k).start()

    def near_copy(src, dst, k, device):
        return pltpu.make_async_remote_copy(
            src, dst, near_send.at[k], near_recv.at[k], device_id=device, device_id_type=MESH
        )

    def near_part(back, c):
        return near.at[pl.ds((REACH - back) * blocks + c * half, half)]

    def hop_one(c):
        return near_copy(own_ref.at[pl.ds(c * half, half)], near_part(2, c), c, follower)

    def hop_two(c):
        return near_copy(near_part(2, c), near_part(4, c), 2 + c, follower)

    def twin_one(c, from_own):
        src = own_ref.at[pl.ds(c * half, half)] if from_own else near_part(2, c)
        return near_copy(src, near_part(1, c), 4 + c, twin)

    def twin_two(c, back):
        return near_copy(near_part(back, c), near_part(3, c), 6 + c, twin)

    def unit(dx, dz, part, of_core):
        to = lax.rem(x + dx + SIDE, SIDE) * SIDE + lax.rem(z + dz + SIDE, SIDE)
        first = (of_core * NODES + to) * CAP
        if part == "full":
            return far.at[pl.ds(pl.multiple_of(first, CAP), CAP)]
        if part == "B":
            first = first + HALF
        return far.at[pl.ds(pl.multiple_of(first, HALF), HALF)]

    def arrives(name):
        (sx, sz), (dx, dz), part = COPIES[name]
        return dx - sx, dz - sz, part

    def send(name):
        (sx, sz), (dx, dz), part = COPIES[name]
        ref, k = unit(dx, dz, part, core), NAMES.index(name)
        return pltpu.make_async_remote_copy(
            ref, ref, unit_send.at[k], unit_recv.at[k], device_id=at(sx, sz), device_id_type=MESH
        )

    def receive(name):
        (sx, sz), _, _ = COPIES[name]
        ref, k = unit(*arrives(name), core), NAMES.index(name)
        return pltpu.make_async_remote_copy(
            ref, ref, unit_send.at[k], unit_recv.at[k], device_id=at(-sx, -sz), device_id_type=MESH
        )

    def share(name, of_core):
        ref = unit(0, 0, "full", of_core) if name == "own" else unit(*arrives(name), of_core)
        k = len(NAMES) if name == "own" else NAMES.index(name)
        return pltpu.make_async_remote_copy(
            ref, ref, twin_send.at[k], twin_recv.at[k], device_id=twin, device_id_type=MESH
        )

    def event(name):
        receive(name).wait_recv()
        for following in THEN[name]:
            send(following).start()
        share(name, core).start()

    wait_input(0)
    wait_input(1)
    to_scalars = pltpu.make_async_copy(table_v, table_s, table_sem.at[0])
    to_scalars.start()
    to_scalars.wait()

    def note_used(h, used):
        for n in range(listed):
            block = table_s[1, h, n] - slab * blocks
            used = tuple(u | (block == j).astype(jnp.int32) for j, u in enumerate(used))
        return used

    used = lax.fori_loop(0, heads, note_used, (jnp.int32(0),) * blocks)
    picked = [jnp.int32(0)] * CAP
    rank = jnp.int32(0)
    for j in range(blocks):
        picked = [jnp.where((used[j] == 1) & (rank == k), j, at_k) for k, at_k in enumerate(picked)]
        rank = rank + used[j]

    wait_input(2)
    wait_input(3)
    for c in (1, 0):
        hop_one(c).start()

    own_unit = pl.multiple_of((core * NODES + node) * CAP, CAP)
    for k in range(CAP):
        for kv in range(2):
            far[own_unit + k, kv] = own_ref[picked[k], kv]

    @pl.when(core == 0)
    def _():
        for c in range(2):
            twin_one(c, True).start()

    for name in ("xm", "zm", "xp"):
        send(name).start()
    share("own", core).start()
    for j in range(blocks):
        for kv in range(2):
            near[REACH * blocks + j, kv] = own_ref[j, kv]

    verticals = table_v[1]
    first_of = verticals // blocks * blocks
    seen = jnp.zeros_like(verticals)
    for h in range(heads):
        for n in range(listed):
            there = table_s[1, h, n] - first_of
            for j in range(blocks - 1):
                seen = seen | jnp.where(there == j, 1 << j, 0)
    before = verticals - first_of
    place = jnp.zeros_like(verticals)
    for j in range(blocks - 1):
        place = place + jnp.where((before > j) & (seen & (1 << j) != 0), 1, 0)
    of_slab = verticals // blocks
    found_v[...] = ((of_slab % 2) * NODES + of_slab // 2) * CAP + place
    to_found = pltpu.make_async_copy(found_v, found_s, table_sem.at[1])
    to_found.start()
    to_found.wait()

    for name in FIRST:
        event(name)
    for c in (1, 0):
        hop_one(c).wait_recv()
        if c == 1:
            hop_two(c).start()
        else:

            @pl.when(core == 1)
            def _():
                hop_two(c).start()

        @pl.when(core == 1)
        def _():
            twin_one(c, False).start()

        @pl.when(core == 0)
        def _():
            twin_two(c, 2).start()

    send("zp").start()
    for name in SECOND:
        event(name)

    @pl.when(core == 1)
    def _():
        for c in (1, 0):
            hop_two(c).wait_recv()
            twin_two(c, 4).start()

    @pl.when(core == 0)
    def _():
        hop_two(1).wait_recv()

    for c in range(2):
        twin_one(c, True).wait_recv()
        twin_two(c, 2).wait_recv()

    factor = math.log2(math.e) / math.sqrt(width)
    causal = lax.broadcasted_iota(jnp.int32, (BLK, BLK), 0) >= lax.broadcasted_iota(
        jnp.int32, (BLK, BLK), 1
    )
    steps = heads * blocks
    base = slab * blocks

    def query(i, h):
        return q_ref[
            pl.ds(pl.multiple_of(i * BLK, BLK), BLK), pl.ds(pl.multiple_of(h * width, width), width)
        ]

    def pair_scores(q, ref, a, b, bias_a, bias_b):
        pair = jnp.dot(
            q, jnp.concatenate([ref[a, 0], ref[b, 0]], axis=1), preferred_element_type=jnp.float32
        )
        return pair[:, :BLK] + bias_a, pair[:, BLK:] + bias_b

    def pair_mix(ref, a, b, wa, wb):
        return jnp.dot(
            jnp.concatenate([wa.astype(jnp.bfloat16), wb.astype(jnp.bfloat16)], axis=1),
            jnp.concatenate([ref[a, 1], ref[b, 1]], axis=0),
            preferred_element_type=jnp.float32,
        )

    def near_entry(i, h, n):
        offset = table_s[0, h, n]
        return REACH * blocks + i - offset, jnp.where(base + i >= offset, 0.0, NEG)

    def near_scores(step, u):
        i, h = step // heads, step % heads
        q = query(i, h)
        own = jnp.dot(q, near[REACH * blocks + i, 0], preferred_element_type=jnp.float32)
        own = jnp.where(causal, own, NEG)
        scores[u][:, :BLK] = own
        top = own
        for n in range(0, listed, 2):
            (a, bias_a), (b, bias_b) = near_entry(i, h, n), near_entry(i, h, n + 1)
            sa, sb = pair_scores(q, near, a, b, bias_a, bias_b)
            scores[u][:, (n + 1) * BLK : (n + 2) * BLK] = sa
            scores[u][:, (n + 2) * BLK : (n + 3) * BLK] = sb
            top = jnp.maximum(top, jnp.maximum(sa, sb))
        top = jnp.max(top, axis=1, keepdims=True) * factor
        top_ref[step] = jnp.broadcast_to(top, (BLK, width))

    def near_mix(step, u):
        i, h = step // heads, step % heads
        top = top_ref[step]

        def weight(n):
            return jnp.exp2(scores[u][:, n * BLK : (n + 1) * BLK] * factor - top)

        total = weight(0)
        mixed = jnp.dot(
            total.astype(jnp.bfloat16), near[REACH * blocks + i, 1], preferred_element_type=jnp.float32
        )
        for n in range(0, listed, 2):
            a, b = near_entry(i, h, n)[0], near_entry(i, h, n + 1)[0]
            wa, wb = weight(n + 1), weight(n + 2)
            total = total + (wa + wb)
            mixed = mixed + pair_mix(near, a, b, wa, wb)
        mixed_ref[step] = mixed
        total_ref[step] = jnp.broadcast_to(jnp.sum(total, axis=1, keepdims=True), (BLK, width))

    def row_block(k):
        late = k // half
        quarter = 2 * ((1 - late) * (1 - high) + late * high) + (k % half) // 2
        return 2 * quarter + k % 2

    def far_bias(own, h, block):
        gap = own - block
        ok = gap > 0
        for n in range(listed):
            ok = ok & (gap != table_s[0, h, n])
        return jnp.where(ok, 0.0, NEG)

    def far_scores(step, u):
        i, h = row_block(step // heads), step % heads
        q = query(i, h)
        top = None
        for n in range(0, listed, 2):
            bias = [far_bias(base + i, h, table_s[1, h, n + d]) for d in range(2)]
            sa, sb = pair_scores(q, far, found_s[h, n], found_s[h, n + 1], *bias)
            scores[u][:, n * BLK : (n + 1) * BLK] = sa
            scores[u][:, (n + 1) * BLK : (n + 2) * BLK] = sb
            both = jnp.maximum(sa, sb)
            top = both if top is None else jnp.maximum(top, both)
        top = jnp.max(top, axis=1, keepdims=True) * factor
        tops[u] = jnp.maximum(jnp.broadcast_to(top, (BLK, width)), top_ref[i * heads + h])

    def far_mix(step, u):
        i, h = row_block(step // heads), step % heads
        top, kept = tops[u], i * heads + h
        scale = jnp.exp2(top_ref[kept] - top)
        total, mixed = None, None
        for n in range(0, listed, 2):
            wa = jnp.exp2(scores[u][:, n * BLK : (n + 1) * BLK] * factor - top)
            wb = jnp.exp2(scores[u][:, (n + 1) * BLK : (n + 2) * BLK] * factor - top)
            total = wa + wb if total is None else total + (wa + wb)
            part = pair_mix(far, found_s[h, n], found_s[h, n + 1], wa, wb)
            mixed = part if mixed is None else mixed + part
        total = jnp.sum(total, axis=1, keepdims=True) + total_ref[kept] * scale
        mixed = mixed + mixed_ref[kept] * scale
        rows = pl.ds(pl.multiple_of(i * BLK, BLK), BLK)
        staged[rows, pl.ds(pl.multiple_of(h * width, width), width)] = (mixed / total).astype(jnp.bfloat16)

    columns = pl.ds(pl.multiple_of(group * heads * width, heads * width), heads * width)

    def out_copy(k):
        i = row_block(k)
        owner, n = i // 2, k % 2
        return pltpu.make_async_remote_copy(
            staged.at[pl.ds(pl.multiple_of(i * BLK, BLK), BLK)],
            out_ref.at[pl.ds(pl.multiple_of(n * BLK, BLK), BLK), columns],
            out_send.at[k], out_recv.at[group * 2 + n],
            device_id=owner_of(owner), device_id_type=MESH,
        )

    def out_keep(k):
        i = row_block(k)
        n = k % 2
        return pltpu.make_async_copy(
            staged.at[pl.ds(pl.multiple_of(i * BLK, BLK), BLK)],
            out_ref.at[pl.ds(pl.multiple_of(n * BLK, BLK), BLK), columns],
            out_local.at[n],
        )

    def kept_here(k):
        return native & (row_block(k) // 2 == head)

    def out_in(of_group, n):
        return pltpu.make_async_remote_copy(
            staged.at[pl.ds(0, BLK)],
            out_ref.at[pl.ds(n * BLK, BLK), pl.ds(of_group * heads * width, heads * width)],
            out_send.at[0], out_recv.at[of_group * 2 + n],
            device_id=worker_of(jnp.int32(of_group)), device_id_type=MESH,
        )

    def send_block(k):
        @pl.when(kept_here(k))
        def _():
            out_keep(k).start()

        @pl.when(jnp.logical_not(kept_here(k)))
        def _():
            out_copy(k).start()

    def near_loop(k, carry):
        for j, names in enumerate(LATER):

            @pl.when(k == j + 1)
            def _():
                for name in names:
                    event(name)

        first = 4 * k
        near_scores(first + 2, 2)
        near_mix(first, 0)
        near_scores(first + 3, 3)
        near_mix(first + 1, 1)
        near_scores(lax.rem(first + 4, steps), 0)
        near_mix(first + 2, 2)
        near_scores(lax.rem(first + 5, steps), 1)
        near_mix(first + 3, 3)
        return carry

    for i in range(blocks):
        wait_input(4 + i)
    near_scores(0, 0)
    near_scores(1, 1)
    lax.fori_loop(0, steps // 4, near_loop, 0)

    for name in NAMES:
        share(name, 1 - core).wait_recv()
    share("own", 1 - core).wait_recv()

    def far_loop(k, carry):
        first = 4 * k
        far_scores(first + 2, 2)
        far_mix(first, 0)
        far_scores(first + 3, 3)
        far_mix(first + 1, 1)
        far_scores(lax.rem(first + 4, steps), 0)
        far_mix(first + 2, 2)
        far_scores(lax.rem(first + 5, steps), 1)
        far_mix(first + 3, 3)

        @pl.when(k % 2 == 1)
        def _():
            send_block(k // 2)

        return carry

    far_scores(0, 0)
    far_scores(1, 1)
    lax.fori_loop(0, steps // 4, far_loop, 0)

    @pl.when(jnp.logical_not(native))
    def _():
        for k in range(len(sources)):
            swap(k).wait_send()

    for c in range(2):
        hop_one(c).wait_send()
        twin_one(c, True).wait_send()
        twin_two(c, 2).wait_send()
    hop_two(1).wait_send()

    @pl.when(core == 1)
    def _():
        hop_two(0).wait_send()

    for name in NAMES:
        send(name).wait_send()
        share(name, core).wait_send()
    share("own", core).wait_send()

    for k in range(blocks):

        @pl.when(kept_here(k))
        def _():
            out_keep(k).wait()

        @pl.when(jnp.logical_not(kept_here(k)))
        def _():
            out_copy(k).wait_send()

    for of_group in range(4):

        @pl.when(jnp.logical_not(native & (group == of_group)))
        def _():
            for n in range(2):
                out_in(of_group, n).wait_recv()


def shards(queries, keys, values, vertical, slash):
    width = keys.shape[1]
    rows = queries.shape[0]
    blocks = rows // BLK
    heads, listed = vertical.shape
    groups = lax.axis_size("head")
    kt = jnp.swapaxes(keys.reshape(blocks, BLK, width), 1, 2)
    v = values.reshape(blocks, BLK, width)
    dma = pltpu.SemaphoreType.DMA
    anywhere = pl.BlockSpec(memory_space=pl.ANY)
    bf16, f32 = jnp.bfloat16, jnp.float32
    inputs = 4 + blocks
    near_width = (listed + 1) * BLK
    return pl.pallas_call(
        functools.partial(layer_kernel, blocks=blocks, heads=heads, width=width, listed=listed),
        in_specs=[anywhere] * 5,
        out_specs=anywhere,
        out_shape=jax.ShapeDtypeStruct((rows // groups, groups * heads * width), bf16),
        scratch_shapes=[
            pltpu.VMEM((2, heads, listed), jnp.int32),
            pltpu.SMEM((2, heads, listed), jnp.int32),
            pltpu.VMEM((heads, listed), jnp.int32),
            pltpu.SMEM((heads, listed), jnp.int32),
            pltpu.VMEM(queries.shape, bf16),
            pltpu.VMEM((blocks, 2, BLK, width), bf16),
            pltpu.VMEM(((REACH + 1) * blocks, 2, BLK, width), bf16),
            pltpu.VMEM((2 * NODES * CAP, 2, BLK, width), bf16),
            pltpu.VMEM(queries.shape, bf16),
            pltpu.VMEM((heads * blocks, BLK, width), f32),
            pltpu.VMEM((heads * blocks, BLK, width), f32),
            pltpu.VMEM((heads * blocks, BLK, width), f32),
            pltpu.VMEM((BLK, near_width), f32),
            pltpu.VMEM((BLK, near_width), f32),
            pltpu.VMEM((BLK, near_width), f32),
            pltpu.VMEM((BLK, near_width), f32),
            pltpu.VMEM((4, BLK, width), f32),
            dma((inputs,)),
            dma((inputs,)),
            dma((inputs,)),
            dma((2,)),
            dma((8,)),
            dma((8,)),
            dma((len(NAMES),)),
            dma((len(NAMES),)),
            dma((len(NAMES) + 1,)),
            dma((len(NAMES) + 1,)),
            dma((2,)),
            dma((blocks,)),
            dma((2 * groups,)),
        ],
        compiler_params=pltpu.CompilerParams(
            collective_id=0, has_side_effects=True, vmem_limit_bytes=62 * 1024 * 1024
        ),
    )(slash, vertical, queries, kt, v)


def solution(mesh):
    in_specs = (
        P("seq", "head"),
        P("seq", "head"),
        P("seq", "head"),
        P("head", None),
        P("head", None),
    )
    out_specs = P(("seq", "head"), None)
    return jax.shard_map(shards, mesh=mesh, in_specs=in_specs, out_specs=out_specs, check_vma=False)
```

```python
import functools
import math

import jax
import jax.numpy as jnp
from jax import lax
from jax.experimental import pallas as pl
from jax.experimental.pallas import tpu as pltpu
from jax.sharding import PartitionSpec as P

BLK = 128
LARGEST_OFFSET = 28
CAP = 4
NEG = -1e30
SIDE = 4
NODES = SIDE * SIDE
REACH = 4
HALF = CAP // 2
MESH = pl.DeviceIdType.MESH

COPIES = {}
COPIES["zm"] = ((0, -1), (0, 0), "full")
COPIES["xp"] = ((1, 0), (0, 0), "full")
COPIES["xm"] = ((-1, 0), (0, 0), "full")
COPIES["zm2"] = ((0, -1), (0, 1), "full")
COPIES["zm3"] = ((0, -1), (0, 2), "full")
COPIES["xm2"] = ((-1, 0), (1, 0), "full")
for d in (1, -1, 2):
    COPIES["xpA", d] = ((1, 0), (0, d), "A")
    COPIES["xmA", d] = ((-1, 0), (0, d), "A")
    COPIES["xmA2", d] = ((-1, 0), (1, d), "A")
    COPIES["zpB", d] = ((0, 1), (d, 0), "B")
    COPIES["zmB", d] = ((0, -1), (d, 0), "B")
    COPIES["zmB2", d] = ((0, -1), (d, 1), "B")
NAMES = list(COPIES)

THEN = {name: [] for name in NAMES}
THEN["zm"] = ["zm2", ("xpA", 1), ("xmA", 1)]
THEN["zm2"] = [("xpA", 2), ("xmA", 2)]
THEN["zm3"] = [("xpA", -1), ("xmA", -1)]
THEN["xm"] = ["xm2", ("zmB", 1)]
THEN["xp"] = [("zmB", -1)]
THEN["xm2"] = [("zmB", 2), ("zpB", 2)]
for d in (1, -1, 2):
    THEN["xmA", d] = [("xmA2", d)]
    THEN["zmB", d] = [("zmB2", d)]

FIRST = ["zm", "xm", "xp"]
SECOND = ["zm2", "xm2", ("zmB", 1), ("xmA", 1), ("xpA", 1), ("zmB", -1)]
LATER = [
    [("xmA", -1), ("xpA", -1)],
    [("zpB", 1), ("zpB", -1)],
    [("xmA", 2), ("zmB", 2)],
    [("xpA", 2), ("zmB2", 1)],
    [("xmA2", 1), ("zmB2", -1)],
    [("xmA2", -1), ("zpB", 2)],
    [("xmA2", 2), ("zmB2", 2)],
]


def layer_kernel(
    slash_ref,
    vertical_ref,
    queries_ref,
    kt_ref,
    v_ref,
    out_ref,
    table_v,
    table_s,
    found_v,
    found_s,
    q_ref,
    own_ref,
    hop_ref,
    near,
    far,
    staged,
    mixed_ref,
    top_ref,
    total_ref,
    scores_0,
    scores_1,
    scores_2,
    scores_3,
    tops,
    load_sem,
    swap_send,
    swap_recv,
    table_sem,
    near_send,
    near_recv,
    unit_send,
    unit_recv,
    twin_send,
    twin_recv,
    out_local,
    out_send,
    out_recv,
    *,
    blocks,
    heads,
    width,
    listed,
):
    seq, head = lax.axis_index("seq"), lax.axis_index("head")
    node, low = seq // 2, seq % 2
    high, core = head // 2, head % 2
    x, z = node // SIDE, node % SIDE
    group, slab = 2 * high + low, 2 * node + core
    native = low == core
    scores = (scores_0, scores_1, scores_2, scores_3)
    half = blocks // 2

    def at(dx, dz):
        to = lax.rem(x + dx + SIDE, SIDE) * SIDE + lax.rem(z + dz + SIDE, SIDE)
        return {"seq": 2 * to + low}

    follower = {"seq": 2 * lax.rem(node + 1, NODES) + low}
    leader = {"seq": 2 * lax.rem(node + NODES - 1, NODES) + low}
    twin = {"head": 2 * high + 1 - core}
    counterpart = {"seq": 2 * node + core, "head": 2 * high + low}

    def owner_of(quarter):
        return {"seq": slab, "head": quarter}

    def worker_of(of_group):
        return {"seq": 2 * node + lax.rem(of_group, 2), "head": 2 * (of_group // 2) + low}

    sources = [slash_ref, vertical_ref]
    targets = [table_v.at[0], table_v.at[1]]
    for c in (1, 0):
        for kv, ref in enumerate((kt_ref, v_ref)):
            part = pl.ds(c * half, half)
            sources.append(ref.at[part])
            targets.append(own_ref.at[part, kv])
    first_query = len(sources)
    for i in range(blocks):
        rows = pl.ds(i * BLK, BLK)
        sources.append(queries_ref.at[rows])
        targets.append(q_ref.at[rows])

    def load(k):
        return pltpu.make_async_copy(sources[k], targets[k], load_sem.at[k])

    def swap(k):
        return pltpu.make_async_remote_copy(
            sources[k], targets[k], swap_send.at[k], swap_recv.at[k],
            device_id=counterpart, device_id_type=MESH,
        )

    def wait_input(k):
        @pl.when(native)
        def _():
            load(k).wait()

        @pl.when(jnp.logical_not(native))
        def _():
            swap(k).wait_recv()

    @pl.when(native)
    def _():
        for k in range(len(sources)):
            load(k).start()

    barrier = pltpu.get_barrier_semaphore()

    def greet(device):
        pl.semaphore_signal(barrier, 1, device_id=device, device_id_type=MESH)

    for device in (at(1, 0), at(-1, 0), at(0, 1), at(0, -1), follower, leader, twin):
        greet(device)
    for k in range(4):

        @pl.when(jnp.logical_not(native & (head == k)))
        def _():
            greet(owner_of(k))

        @pl.when(jnp.logical_not(native & (group == k)))
        def _():
            greet(worker_of(jnp.int32(k)))

    @pl.when(jnp.logical_not(native))
    def _():
        greet(counterpart)

    pl.semaphore_wait(barrier, 7 + 6 + 3 * (low - core) * (low - core))

    @pl.when(jnp.logical_not(native))
    def _():
        for k in range(len(sources)):
            swap(k).start()

    def near_copy(src, dst, k, device):
        return pltpu.make_async_remote_copy(
            src, dst, near_send.at[k], near_recv.at[k], device_id=device, device_id_type=MESH
        )

    def near_part(back, c):
        return near.at[pl.ds((REACH - back) * blocks + c * half, half)]

    def hop_one(c):
        part = pl.ds(c * half, half)
        return near_copy(own_ref.at[part], hop_ref.at[part], c, follower)

    def hop_two(c):
        return near_copy(hop_ref.at[pl.ds(c * half, half)], near_part(4, c), 2 + c, follower)

    def twin_one(c, from_own):
        src = (own_ref if from_own else hop_ref).at[pl.ds(c * half, half)]
        return near_copy(src, near_part(1, c), 4 + c, twin)

    def twin_two(c, from_hop):
        src = hop_ref.at[pl.ds(c * half, half)] if from_hop else near_part(4, c)
        return near_copy(src, near_part(3, c), 6 + c, twin)

    def unit(dx, dz, part, of_core):
        to = lax.rem(x + dx + SIDE, SIDE) * SIDE + lax.rem(z + dz + SIDE, SIDE)
        first = (of_core * NODES + to) * CAP
        if part == "full":
            return far.at[pl.ds(pl.multiple_of(first, CAP), CAP)]
        if part == "B":
            first = first + HALF
        return far.at[pl.ds(pl.multiple_of(first, HALF), HALF)]

    def arrives(name):
        (sx, sz), (dx, dz), part = COPIES[name]
        return dx - sx, dz - sz, part

    def send(name):
        (sx, sz), (dx, dz), part = COPIES[name]
        ref, k = unit(dx, dz, part, core), NAMES.index(name)
        return pltpu.make_async_remote_copy(
            ref, ref, unit_send.at[k], unit_recv.at[k], device_id=at(sx, sz), device_id_type=MESH
        )

    def receive(name):
        (sx, sz), _, _ = COPIES[name]
        ref, k = unit(*arrives(name), core), NAMES.index(name)
        return pltpu.make_async_remote_copy(
            ref, ref, unit_send.at[k], unit_recv.at[k], device_id=at(-sx, -sz), device_id_type=MESH
        )

    def share(name, of_core):
        ref = unit(0, 0, "full", of_core) if name == "own" else unit(*arrives(name), of_core)
        k = len(NAMES) if name == "own" else NAMES.index(name)
        return pltpu.make_async_remote_copy(
            ref, ref, twin_send.at[k], twin_recv.at[k], device_id=twin, device_id_type=MESH
        )

    def event(name):
        receive(name).wait_recv()
        for following in THEN[name]:
            send(following).start()
        share(name, core).start()

    wait_input(0)
    wait_input(1)
    to_scalars = pltpu.make_async_copy(table_v, table_s, table_sem.at[0])
    to_scalars.start()
    to_scalars.wait()

    def note_used(h, used):
        for n in range(listed):
            block = table_s[1, h, n] - (slab - 2) * blocks
            used = tuple(
                u | (block == (j if j < blocks else j + blocks)).astype(jnp.int32)
                for j, u in enumerate(used)
            )
        return used

    used = lax.fori_loop(0, heads, note_used, (jnp.int32(0),) * (2 * blocks))

    def choose(used):
        picked, rank = [jnp.int32(0)] * CAP, jnp.int32(0)
        for j in range(blocks):
            picked = [
                jnp.where((used[j] == 1) & (rank == k), j, at_k) for k, at_k in enumerate(picked)
            ]
            rank = rank + used[j]
        return picked

    picked_before, picked = choose(used[:blocks]), choose(used[blocks:])

    verticals = table_v[1]
    first_of = verticals // blocks * blocks
    seen = jnp.zeros_like(verticals)
    for h in range(heads):
        for n in range(listed):
            there = table_s[1, h, n] - first_of
            for j in range(blocks - 1):
                seen = seen | jnp.where(there == j, 1 << j, 0)
    before = verticals - first_of
    place = jnp.zeros_like(verticals)
    for j in range(blocks - 1):
        place = place + jnp.where((before > j) & (seen & (1 << j) != 0), 1, 0)
    of_slab = verticals // blocks
    found_v[...] = ((of_slab % 2) * NODES + of_slab // 2) * CAP + place
    to_found = pltpu.make_async_copy(found_v, found_s, table_sem.at[1])
    to_found.start()

    def pack(src, node_of, picked):
        first = pl.multiple_of((core * NODES + node_of) * CAP, CAP)
        for k in range(CAP):
            for kv in range(2):
                far[first + k, kv] = src[picked[k], kv]

    for c in (1, 0):
        for k in range(2):
            wait_input(2 + 2 * (1 - c) + k)
        hop_one(c).start()

        @pl.when(core == 0)
        def _():
            twin_one(c, True).start()

    pack(own_ref, node, picked)
    for j in range(blocks):
        for kv in range(2):
            near[REACH * blocks + j, kv] = own_ref[j, kv]
    for name in ("zm", "xm", "xp"):
        send(name).start()
    share("own", core).start()
    to_found.wait()

    for name in FIRST:
        event(name)
    for c in (1, 0):
        hop_one(c).wait_recv()
        if c == 1:
            hop_two(c).start()
        else:

            @pl.when(core == 1)
            def _():
                hop_two(c).start()

        @pl.when(core == 1)
        def _():
            twin_one(c, False).start()

        @pl.when(core == 0)
        def _():
            twin_two(c, True).start()

    @pl.when(z > 0)
    def _():
        pack(hop_ref, x * SIDE + z - 1, picked_before)

    for j in range(blocks):
        for kv in range(2):
            near[2 * blocks + j, kv] = hop_ref[j, kv]

    @pl.when(z > 0)
    def _():
        for following in THEN["zm3"]:
            send(following).start()
        share("zm3", core).start()

    for d in (1, -1):
        send(("zpB", d)).start()
    for name in SECOND:
        event(name)
        if name == "zm2":

            @pl.when(z == 1)
            def _():
                send("zm3").start()

    @pl.when(core == 1)
    def _():
        for c in (1, 0):
            hop_two(c).wait_recv()
            twin_two(c, False).start()

    @pl.when(core == 0)
    def _():
        hop_two(1).wait_recv()

    for c in range(2):
        twin_one(c, True).wait_recv()
        twin_two(c, True).wait_recv()

    @pl.when(z == 0)
    def _():
        event("zm3")

    factor = math.log2(math.e) / math.sqrt(width)
    causal = lax.broadcasted_iota(jnp.int32, (BLK, BLK), 0) >= lax.broadcasted_iota(
        jnp.int32, (BLK, BLK), 1
    )
    steps = heads * blocks
    base = slab * blocks

    def query(i, h):
        return q_ref[
            pl.ds(i * BLK if isinstance(i, int) else pl.multiple_of(i * BLK, BLK), BLK),
            pl.ds(pl.multiple_of(h * width, width), width),
        ]

    def pair_scores(q, ref, a, b, bias_a, bias_b):
        pair = jnp.dot(
            q, jnp.concatenate([ref[a, 0], ref[b, 0]], axis=1), preferred_element_type=jnp.float32
        )
        return pair[:, :BLK] + bias_a, pair[:, BLK:] + bias_b

    def pair_mix(ref, a, b, wa, wb):
        return jnp.dot(
            jnp.concatenate([wa.astype(jnp.bfloat16), wb.astype(jnp.bfloat16)], axis=1),
            jnp.concatenate([ref[a, 1], ref[b, 1]], axis=0),
            preferred_element_type=jnp.float32,
        )

    def near_entry(i, h, n):
        offset = table_s[0, h, n]
        return REACH * blocks + i - offset, jnp.where(base + i >= offset, 0.0, NEG)

    def near_scores(i, h, u):
        step = i * heads + h
        q = query(i, h)
        own = jnp.dot(q, near[REACH * blocks + i, 0], preferred_element_type=jnp.float32)
        own = jnp.where(causal, own, NEG)
        scores[u][:, :BLK] = own
        top = own
        for n in range(0, listed, 2):
            (a, bias_a), (b, bias_b) = near_entry(i, h, n), near_entry(i, h, n + 1)
            sa, sb = pair_scores(q, near, a, b, bias_a, bias_b)
            scores[u][:, (n + 1) * BLK : (n + 2) * BLK] = sa
            scores[u][:, (n + 2) * BLK : (n + 3) * BLK] = sb
            top = jnp.maximum(top, jnp.maximum(sa, sb))
        top = jnp.max(top, axis=1, keepdims=True) * factor
        top_ref[step] = jnp.broadcast_to(top, (BLK, width))

    def near_mix(step, u):
        i, h = step // heads, step % heads
        top = top_ref[step]

        def weight(n):
            return jnp.exp2(scores[u][:, n * BLK : (n + 1) * BLK] * factor - top)

        total = weight(0)
        mixed = jnp.dot(
            total.astype(jnp.bfloat16), near[REACH * blocks + i, 1], preferred_element_type=jnp.float32
        )
        for n in range(0, listed, 2):
            a, b = near_entry(i, h, n)[0], near_entry(i, h, n + 1)[0]
            wa, wb = weight(n + 1), weight(n + 2)
            total = total + (wa + wb)
            mixed = mixed + pair_mix(near, a, b, wa, wb)
        mixed_ref[step] = mixed
        total_ref[step] = jnp.broadcast_to(jnp.sum(total, axis=1, keepdims=True), (BLK, width))

    def row_block(k):
        late = k // half
        quarter = 2 * ((1 - late) * (1 - high) + late * high) + (k % half) // 2
        return 2 * quarter + k % 2

    def far_bias(own, h, block):
        gap = own - block
        ok = gap > 0
        for n in range(listed):
            ok = ok & (gap != table_s[0, h, n])
        return jnp.where(ok, 0.0, NEG)

    def far_scores(step, u):
        i, h = row_block(step // heads), step % heads
        q = query(i, h)
        top = None
        for n in range(0, listed, 2):
            bias = [far_bias(base + i, h, table_s[1, h, n + d]) for d in range(2)]
            sa, sb = pair_scores(q, far, found_s[h, n], found_s[h, n + 1], *bias)
            scores[u][:, n * BLK : (n + 1) * BLK] = sa
            scores[u][:, (n + 1) * BLK : (n + 2) * BLK] = sb
            both = jnp.maximum(sa, sb)
            top = both if top is None else jnp.maximum(top, both)
        top = jnp.max(top, axis=1, keepdims=True) * factor
        tops[u] = jnp.maximum(jnp.broadcast_to(top, (BLK, width)), top_ref[i * heads + h])

    def far_mix(step, u):
        i, h = row_block(step // heads), step % heads
        top, kept = tops[u], i * heads + h
        scale = jnp.exp2(top_ref[kept] - top)
        total, mixed = None, None
        for n in range(0, listed, 2):
            wa = jnp.exp2(scores[u][:, n * BLK : (n + 1) * BLK] * factor - top)
            wb = jnp.exp2(scores[u][:, (n + 1) * BLK : (n + 2) * BLK] * factor - top)
            total = wa + wb if total is None else total + (wa + wb)
            part = pair_mix(far, found_s[h, n], found_s[h, n + 1], wa, wb)
            mixed = part if mixed is None else mixed + part
        total = jnp.sum(total, axis=1, keepdims=True) + total_ref[kept] * scale
        mixed = mixed + mixed_ref[kept] * scale
        rows = pl.ds(pl.multiple_of(i * BLK, BLK), BLK)
        staged[rows, pl.ds(pl.multiple_of(h * width, width), width)] = (mixed / total).astype(jnp.bfloat16)

    columns = pl.ds(pl.multiple_of(group * heads * width, heads * width), heads * width)

    def out_copy(k):
        i = row_block(k)
        owner, n = i // 2, k % 2
        return pltpu.make_async_remote_copy(
            staged.at[pl.ds(pl.multiple_of(i * BLK, BLK), BLK)],
            out_ref.at[pl.ds(pl.multiple_of(n * BLK, BLK), BLK), columns],
            out_send.at[k], out_recv.at[group * 2 + n],
            device_id=owner_of(owner), device_id_type=MESH,
        )

    def out_keep(k):
        i = row_block(k)
        n = k % 2
        return pltpu.make_async_copy(
            staged.at[pl.ds(pl.multiple_of(i * BLK, BLK), BLK)],
            out_ref.at[pl.ds(pl.multiple_of(n * BLK, BLK), BLK), columns],
            out_local.at[n],
        )

    def kept_here(k):
        return native & (row_block(k) // 2 == head)

    def out_in(of_group, n):
        return pltpu.make_async_remote_copy(
            staged.at[pl.ds(0, BLK)],
            out_ref.at[pl.ds(n * BLK, BLK), pl.ds(of_group * heads * width, heads * width)],
            out_send.at[0], out_recv.at[of_group * 2 + n],
            device_id=worker_of(jnp.int32(of_group)), device_id_type=MESH,
        )

    def send_block(k):
        @pl.when(kept_here(k))
        def _():
            out_keep(k).start()

        @pl.when(jnp.logical_not(kept_here(k)))
        def _():
            out_copy(k).start()

    def near_steps(i, k, carry):
        first = i * heads + 4 * k
        for u in range(4):
            near_scores(i, 4 * k + u, u)
            near_mix(lax.rem(first + steps + u - 2, steps), (u + 2) % 4)
        return carry

    for i in range(blocks):
        wait_input(first_query + i)
        lax.fori_loop(0, heads // 4, functools.partial(near_steps, i), 0)
        if i < len(LATER):
            for name in LATER[i]:
                event(name)
    for u in (2, 3):
        near_mix(steps - 4 + u, u)

    for name in NAMES:
        share(name, 1 - core).wait_recv()
    share("own", 1 - core).wait_recv()

    def far_loop(k, carry):
        first = 4 * k
        far_scores(first + 2, 2)
        far_mix(first, 0)
        far_scores(first + 3, 3)
        far_mix(first + 1, 1)
        far_scores(lax.rem(first + 4, steps), 0)
        far_mix(first + 2, 2)
        far_scores(lax.rem(first + 5, steps), 1)
        far_mix(first + 3, 3)

        @pl.when(k % 2 == 1)
        def _():
            send_block(k // 2)

        return carry

    far_scores(0, 0)
    far_scores(1, 1)
    lax.fori_loop(0, steps // 4, far_loop, 0)

    @pl.when(jnp.logical_not(native))
    def _():
        for k in range(len(sources)):
            swap(k).wait_send()

    for c in range(2):
        hop_one(c).wait_send()
        twin_one(c, True).wait_send()
        twin_two(c, True).wait_send()
    hop_two(1).wait_send()

    @pl.when(core == 1)
    def _():
        hop_two(0).wait_send()

    for name in NAMES:
        share(name, core).wait_send()
        if name != "zm3":
            send(name).wait_send()

    @pl.when(z == 1)
    def _():
        send("zm3").wait_send()

    share("own", core).wait_send()

    for k in range(blocks):

        @pl.when(kept_here(k))
        def _():
            out_keep(k).wait()

        @pl.when(jnp.logical_not(kept_here(k)))
        def _():
            out_copy(k).wait_send()

    for of_group in range(4):

        @pl.when(jnp.logical_not(native & (group == of_group)))
        def _():
            for n in range(2):
                out_in(of_group, n).wait_recv()


def shards(queries, keys, values, vertical, slash):
    width = keys.shape[1]
    rows = queries.shape[0]
    blocks = rows // BLK
    heads, listed = vertical.shape
    groups = lax.axis_size("head")
    kt = jnp.swapaxes(keys.reshape(blocks, BLK, width), 1, 2)
    v = values.reshape(blocks, BLK, width)
    dma = pltpu.SemaphoreType.DMA
    anywhere = pl.BlockSpec(memory_space=pl.ANY)
    bf16, f32 = jnp.bfloat16, jnp.float32
    inputs = 6 + blocks
    near_width = (listed + 1) * BLK
    return pl.pallas_call(
        functools.partial(layer_kernel, blocks=blocks, heads=heads, width=width, listed=listed),
        in_specs=[anywhere] * 5,
        out_specs=anywhere,
        out_shape=jax.ShapeDtypeStruct((rows // groups, groups * heads * width), bf16),
        scratch_shapes=[
            pltpu.VMEM((2, heads, listed), jnp.int32),
            pltpu.SMEM((2, heads, listed), jnp.int32),
            pltpu.VMEM((heads, listed), jnp.int32),
            pltpu.SMEM((heads, listed), jnp.int32),
            pltpu.VMEM(queries.shape, bf16),
            pltpu.VMEM((blocks, 2, BLK, width), bf16),
            pltpu.VMEM((blocks, 2, BLK, width), bf16),
            pltpu.VMEM(((REACH + 1) * blocks, 2, BLK, width), bf16),
            pltpu.VMEM((2 * NODES * CAP, 2, BLK, width), bf16),
            pltpu.VMEM(queries.shape, bf16),
            pltpu.VMEM((heads * blocks, BLK, width), f32),
            pltpu.VMEM((heads * blocks, BLK, width), f32),
            pltpu.VMEM((heads * blocks, BLK, width), f32),
            pltpu.VMEM((BLK, near_width), f32),
            pltpu.VMEM((BLK, near_width), f32),
            pltpu.VMEM((BLK, near_width), f32),
            pltpu.VMEM((BLK, near_width), f32),
            pltpu.VMEM((4, BLK, width), f32),
            dma((inputs,)),
            dma((inputs,)),
            dma((inputs,)),
            dma((2,)),
            dma((8,)),
            dma((8,)),
            dma((len(NAMES),)),
            dma((len(NAMES),)),
            dma((len(NAMES) + 1,)),
            dma((len(NAMES) + 1,)),
            dma((2,)),
            dma((blocks,)),
            dma((2 * groups,)),
        ],
        compiler_params=pltpu.CompilerParams(
            collective_id=0, has_side_effects=True, vmem_limit_bytes=62 * 1024 * 1024
        ),
    )(slash, vertical, queries, kt, v)


def solution(mesh):
    in_specs = (
        P("seq", "head"),
        P("seq", "head"),
        P("seq", "head"),
        P("head", None),
        P("head", None),
    )
    out_specs = P(("seq", "head"), None)
    return jax.shard_map(shards, mesh=mesh, in_specs=in_specs, out_specs=out_specs, check_vma=False)
```

```python
import functools
import math

import jax
import jax.numpy as jnp
from jax import lax
from jax.experimental import pallas as pl
from jax.experimental.pallas import tpu as pltpu
from jax.sharding import PartitionSpec as P

BLK = 128
LARGEST_OFFSET = 28
CAP = 4
NEG = -1e30
SIDE = 4
NODES = SIDE * SIDE
REACH = 4
HALF = CAP // 2
MESH = pl.DeviceIdType.MESH

COPIES = {}
COPIES["zm"] = ((0, -1), (0, 0), "full")
COPIES["xp"] = ((1, 0), (0, 0), "full")
COPIES["xm"] = ((-1, 0), (0, 0), "full")
COPIES["zm2"] = ((0, -1), (0, 1), "full")
COPIES["zm3"] = ((0, -1), (0, 2), "full")
COPIES["xm2"] = ((-1, 0), (1, 0), "full")
for d in (1, -1, 2):
    COPIES["xpA", d] = ((1, 0), (0, d), "A")
    COPIES["xmA", d] = ((-1, 0), (0, d), "A")
    COPIES["xmA2", d] = ((-1, 0), (1, d), "A")
    COPIES["zpB", d] = ((0, 1), (d, 0), "B")
    COPIES["zmB", d] = ((0, -1), (d, 0), "B")
    COPIES["zmB2", d] = ((0, -1), (d, 1), "B")
NAMES = list(COPIES)

THEN = {name: [] for name in NAMES}
THEN["zm"] = ["zm2", ("xpA", 1), ("xmA", 1)]
THEN["zm2"] = [("xpA", 2), ("xmA", 2)]
THEN["zm3"] = [("xpA", -1), ("xmA", -1)]
THEN["xm"] = ["xm2", ("zmB", 1)]
THEN["xp"] = [("zmB", -1), ("zpB", -1)]
THEN["xm2"] = [("zmB", 2), ("zpB", 2)]
for d in (1, -1, 2):
    THEN["xmA", d] = [("xmA2", d)]
    THEN["zmB", d] = [("zmB2", d)]

FIRST = ["zm", "xm"]
SECOND = ["zm2", "xm2", ("zmB", 1), ("xmA", 1)]
THIRD = [("xmA", 2), ("zmB", 2)]
LATER = [
    [("xmA", -1), ("zmB", -1), ("zmB2", 1), ("xmA2", 1)],
    [("xmA2", 2), ("zmB2", 2)],
    [("xmA2", -1), ("zmB2", -1)],
    [(name, d) for d in (1, -1, 2) for name in ("xpA", "zpB")],
]


def layer_kernel(
    slash_ref,
    vertical_ref,
    queries_ref,
    kt_ref,
    v_ref,
    out_ref,
    table_v,
    table_s,
    found_v,
    found_s,
    picked_s,
    q_ref,
    own_ref,
    hop_ref,
    near,
    far,
    staged,
    mixed_ref,
    top_ref,
    total_ref,
    scores_0,
    scores_1,
    scores_2,
    scores_3,
    weights_0,
    weights_1,
    weights_2,
    weights_3,
    tops,
    load_sem,
    swap_send,
    swap_recv,
    table_sem,
    near_send,
    near_recv,
    unit_send,
    unit_recv,
    twin_send,
    twin_recv,
    out_local,
    out_send,
    out_recv,
    *,
    blocks,
    heads,
    width,
    listed,
):
    seq, head = lax.axis_index("seq"), lax.axis_index("head")
    node, low = seq // 2, seq % 2
    high, core = head // 2, head % 2
    x, z = node // SIDE, node % SIDE
    group, slab = 2 * high + low, 2 * node + core
    native = low == core
    scores = (scores_0, scores_1, scores_2, scores_3)
    weights = (weights_0, weights_1, weights_2, weights_3)
    half = blocks // 2

    def at(dx, dz):
        to = lax.rem(x + dx + SIDE, SIDE) * SIDE + lax.rem(z + dz + SIDE, SIDE)
        return {"seq": 2 * to + low}

    follower = {"seq": 2 * lax.rem(node + 1, NODES) + low}
    leader = {"seq": 2 * lax.rem(node + NODES - 1, NODES) + low}
    twin = {"head": 2 * high + 1 - core}
    counterpart = {"seq": 2 * node + core, "head": 2 * high + low}

    def owner_of(quarter):
        return {"seq": slab, "head": quarter}

    def worker_of(of_group):
        return {"seq": 2 * node + lax.rem(of_group, 2), "head": 2 * (of_group // 2) + low}

    def row_block(k):
        late = k // half
        quarter = 2 * ((1 - late) * (1 - high) + late * high) + (k % half) // 2
        return 2 * quarter + k % 2

    sources = [slash_ref, vertical_ref]
    targets = [table_v.at[0], table_v.at[1]]
    for c in (1, 0):
        for kv, ref in enumerate((kt_ref, v_ref)):
            part = pl.ds(c * half, half)
            sources.append(ref.at[part])
            targets.append(own_ref.at[part, kv])
    first_query = len(sources)
    for k in range(blocks):
        rows = pl.ds(pl.multiple_of(row_block(k) * BLK, BLK), BLK)
        sources.append(queries_ref.at[rows])
        targets.append(q_ref.at[rows])

    def load(k):
        return pltpu.make_async_copy(sources[k], targets[k], load_sem.at[k])

    def swap(k):
        return pltpu.make_async_remote_copy(
            sources[k], targets[k], swap_send.at[k], swap_recv.at[k],
            device_id=counterpart, device_id_type=MESH,
        )

    def wait_input(k):
        @pl.when(native)
        def _():
            load(k).wait()

        @pl.when(jnp.logical_not(native))
        def _():
            swap(k).wait_recv()

    def prepare(wait_table):
        for k in range(2):
            wait_table(k)
        to_scalars = pltpu.make_async_copy(table_v, table_s, table_sem.at[0])
        to_scalars.start()
        to_scalars.wait()

        def note_used(h, used):
            for n in range(listed):
                block = table_s[1, h, n] - (slab - 2) * blocks
                used = tuple(
                    u | (block == (j if j < blocks else j + blocks)).astype(jnp.int32)
                    for j, u in enumerate(used)
                )
            return used

        used = lax.fori_loop(0, heads, note_used, (jnp.int32(0),) * (2 * blocks))

        def choose(used):
            picked, rank = [jnp.int32(0)] * CAP, jnp.int32(0)
            for j in range(blocks):
                picked = [
                    jnp.where((used[j] == 1) & (rank == k), j, at_k) for k, at_k in enumerate(picked)
                ]
                rank = rank + used[j]
            return picked

        for c in range(2):
            for k, block in enumerate(choose(used[c * blocks : (c + 1) * blocks])):
                picked_s[c, k] = block

        verticals = table_v[1]
        first_of = verticals // blocks * blocks
        seen = jnp.zeros_like(verticals)
        for h in range(heads):
            for n in range(listed):
                there = table_s[1, h, n] - first_of
                for j in range(blocks - 1):
                    seen = seen | jnp.where(there == j, 1 << j, 0)
        before = verticals - first_of
        place = jnp.zeros_like(verticals)
        for j in range(blocks - 1):
            place = place + jnp.where((before > j) & (seen & (1 << j) != 0), 1, 0)
        of_slab = verticals // blocks
        found_v[...] = ((of_slab % 2) * NODES + of_slab // 2) * CAP + place
        to_found = pltpu.make_async_copy(found_v, found_s, table_sem.at[1])
        to_found.start()
        to_found.wait()

    @pl.when(native)
    def _():
        for k in range(len(sources)):
            load(k).start()

    barrier = pltpu.get_barrier_semaphore()

    def greet(device):
        pl.semaphore_signal(barrier, 1, device_id=device, device_id_type=MESH)

    for device in (at(1, 0), at(-1, 0), at(0, 1), at(0, -1), follower, leader, twin):
        greet(device)
    for k in range(4):

        @pl.when(jnp.logical_not(native & (head == k)))
        def _():
            greet(owner_of(k))

        @pl.when(jnp.logical_not(native & (group == k)))
        def _():
            greet(worker_of(jnp.int32(k)))

    @pl.when(jnp.logical_not(native))
    def _():
        greet(counterpart)

    @pl.when(native)
    def _():
        prepare(lambda k: load(k).wait())

    pl.semaphore_wait(barrier, 7 + 6 + 3 * (low - core) * (low - core))

    @pl.when(jnp.logical_not(native))
    def _():
        for k in range(len(sources)):
            swap(k).start()
        prepare(lambda k: swap(k).wait_recv())

    def near_copy(src, dst, k, device):
        return pltpu.make_async_remote_copy(
            src, dst, near_send.at[k], near_recv.at[k], device_id=device, device_id_type=MESH
        )

    def near_part(back, c):
        return near.at[pl.ds((REACH - back) * blocks + c * half, half)]

    def hop_one(c):
        part = pl.ds(c * half, half)
        return near_copy(own_ref.at[part], hop_ref.at[part], c, follower)

    def hop_two(c):
        return near_copy(hop_ref.at[pl.ds(c * half, half)], near_part(4, c), 2 + c, follower)

    def twin_one(c, from_own):
        src = (own_ref if from_own else hop_ref).at[pl.ds(c * half, half)]
        return near_copy(src, near_part(1, c), 4 + c, twin)

    def twin_two(c, from_hop):
        src = hop_ref.at[pl.ds(c * half, half)] if from_hop else near_part(4, c)
        return near_copy(src, near_part(3, c), 6 + c, twin)

    def unit(dx, dz, part, of_core):
        to = lax.rem(x + dx + SIDE, SIDE) * SIDE + lax.rem(z + dz + SIDE, SIDE)
        first = (of_core * NODES + to) * CAP
        if part == "full":
            return far.at[pl.ds(pl.multiple_of(first, CAP), CAP)]
        if part == "B":
            first = first + HALF
        return far.at[pl.ds(pl.multiple_of(first, HALF), HALF)]

    def arrives(name):
        (sx, sz), (dx, dz), part = COPIES[name]
        return dx - sx, dz - sz, part

    def send(name):
        (sx, sz), (dx, dz), part = COPIES[name]
        ref, k = unit(dx, dz, part, core), NAMES.index(name)
        return pltpu.make_async_remote_copy(
            ref, ref, unit_send.at[k], unit_recv.at[k], device_id=at(sx, sz), device_id_type=MESH
        )

    def receive(name):
        (sx, sz), _, _ = COPIES[name]
        ref, k = unit(*arrives(name), core), NAMES.index(name)
        return pltpu.make_async_remote_copy(
            ref, ref, unit_send.at[k], unit_recv.at[k], device_id=at(-sx, -sz), device_id_type=MESH
        )

    def share(name, of_core):
        ref = unit(0, 0, "full", of_core) if name == "own" else unit(*arrives(name), of_core)
        k = len(NAMES) if name == "own" else NAMES.index(name)
        return pltpu.make_async_remote_copy(
            ref, ref, twin_send.at[k], twin_recv.at[k], device_id=twin, device_id_type=MESH
        )

    def start(name):
        if name[0] == "zpB":
            return
        if name == "xp" or name[0] == "xpA":

            @pl.when(z < SIDE - 1)
            def _():
                send(name).start()

        else:
            send(name).start()

    def event(name):
        receive(name).wait_recv()
        for following in THEN[name]:
            start(following)
        share(name, core).start()

    def pack(src, node_of, c):
        first = pl.multiple_of((core * NODES + node_of) * CAP, CAP)
        for k in range(CAP):
            for kv in range(2):
                far[first + k, kv] = src[picked_s[c, k], kv]

    for c in (1, 0):
        for k in range(2):
            wait_input(2 + 2 * (1 - c) + k)
        hop_one(c).start()

        @pl.when(core == 0)
        def _():
            twin_one(c, True).start()

    pack(own_ref, node, 1)
    for j in range(blocks):
        for kv in range(2):
            near[REACH * blocks + j, kv] = own_ref[j, kv]
    for name in ("zm", "xm", "xp"):
        start(name)
    share("own", core).start()

    for name in FIRST:
        event(name)
    for c in (1, 0):
        hop_one(c).wait_recv()
        if c == 1:
            hop_two(c).start()
        else:

            @pl.when(core == 1)
            def _():
                hop_two(c).start()

        @pl.when(core == 1)
        def _():
            twin_one(c, False).start()

        @pl.when(core == 0)
        def _():
            twin_two(c, True).start()

    @pl.when(z > 0)
    def _():
        pack(hop_ref, x * SIDE + z - 1, 0)

    for j in range(blocks):
        for kv in range(2):
            near[2 * blocks + j, kv] = hop_ref[j, kv]

    @pl.when(z > 0)
    def _():
        for following in THEN["zm3"]:
            start(following)
        share("zm3", core).start()

    @pl.when(z == SIDE - 1)
    def _():
        send("xp").start()

    @pl.when(z < SIDE - 1)
    def _():
        event("xp")

    for name in SECOND:
        event(name)
        if name == "zm2":

            @pl.when(z == 1)
            def _():
                send("zm3").start()

    @pl.when(z == SIDE - 1)
    def _():
        event("xp")

    @pl.when(z == 0)
    def _():
        event("zm3")

    for name in THIRD:
        event(name)

    @pl.when(core == 1)
    def _():
        for c in (1, 0):
            hop_two(c).wait_recv()
            twin_two(c, False).start()

    @pl.when(core == 0)
    def _():
        hop_two(1).wait_recv()

    for c in range(2):
        twin_one(c, True).wait_recv()
        twin_two(c, True).wait_recv()

    for d in (1, -1, 2):
        send(("zpB", d)).start()

    @pl.when(z == SIDE - 1)
    def _():
        for d in (1, -1, 2):
            send(("xpA", d)).start()

    factor = math.log2(math.e) / math.sqrt(width)
    causal = lax.broadcasted_iota(jnp.int32, (BLK, BLK), 0) >= lax.broadcasted_iota(
        jnp.int32, (BLK, BLK), 1
    )
    steps = heads * blocks
    base = slab * blocks

    def query(i, h):
        return q_ref[
            pl.ds(pl.multiple_of(i * BLK, BLK), BLK),
            pl.ds(pl.multiple_of(h * width, width), width),
        ]

    def pair_scores(q, ref, a, b, bias_a, bias_b):
        pair = jnp.dot(
            q, jnp.concatenate([ref[a, 0], ref[b, 0]], axis=1), preferred_element_type=jnp.float32
        )
        return pair[:, :BLK] + bias_a, pair[:, BLK:] + bias_b

    def pair_mix(u, n, ref, a, b):
        return jnp.dot(
            weights[u][:, n * BLK : (n + 2) * BLK],
            jnp.concatenate([ref[a, 1], ref[b, 1]], axis=0),
            preferred_element_type=jnp.float32,
        )

    def row_top(u, count):
        top = scores[u][:, :BLK]
        for n in range(1, count):
            top = jnp.maximum(top, scores[u][:, n * BLK : (n + 1) * BLK])
        return jnp.broadcast_to(jnp.max(top, axis=1, keepdims=True) * factor, (BLK, width))

    def weigh(u, count, top):
        total = None
        for n in range(count):
            w = jnp.exp2(scores[u][:, n * BLK : (n + 1) * BLK] * factor - top)
            total = w if total is None else total + w
            weights[u][:, n * BLK : (n + 1) * BLK] = w.astype(jnp.bfloat16)
        return jnp.broadcast_to(jnp.sum(total, axis=1, keepdims=True), (BLK, width))

    def near_entry(i, h, n):
        offset = table_s[0, h, n]
        return REACH * blocks + i - offset, jnp.where(base + i >= offset, 0.0, NEG)

    def near_scores(k, h, u):
        i = row_block(k)
        q = query(i, h)
        own = jnp.dot(q, near[REACH * blocks + i, 0], preferred_element_type=jnp.float32)
        scores[u][:, :BLK] = jnp.where(causal, own, NEG)
        for n in range(0, listed, 2):
            (a, bias_a), (b, bias_b) = near_entry(i, h, n), near_entry(i, h, n + 1)
            sa, sb = pair_scores(q, near, a, b, bias_a, bias_b)
            scores[u][:, (n + 1) * BLK : (n + 2) * BLK] = sa
            scores[u][:, (n + 2) * BLK : (n + 3) * BLK] = sb

    def near_weigh(step, u):
        top_ref[step] = row_top(u, listed + 1)
        total_ref[step] = weigh(u, listed + 1, top_ref[step])

    def near_mix(step, u):
        i, h = row_block(step // heads), step % heads
        mixed = jnp.dot(
            weights[u][:, :BLK], near[REACH * blocks + i, 1], preferred_element_type=jnp.float32
        )
        for n in range(0, listed, 2):
            a, b = near_entry(i, h, n)[0], near_entry(i, h, n + 1)[0]
            mixed = mixed + pair_mix(u, n + 1, near, a, b)
        mixed_ref[step] = mixed

    def far_bias(own, h, block):
        gap = own - block
        ok = gap > 0
        for n in range(listed):
            ok = ok & (gap != table_s[0, h, n])
        return jnp.where(ok, 0.0, NEG)

    def far_scores(step, u):
        i, h = row_block(step // heads), step % heads
        q = query(i, h)
        top = None
        for n in range(0, listed, 2):
            bias = [far_bias(base + i, h, table_s[1, h, n + d]) for d in range(2)]
            sa, sb = pair_scores(q, far, found_s[h, n], found_s[h, n + 1], *bias)
            scores[u][:, n * BLK : (n + 1) * BLK] = sa
            scores[u][:, (n + 1) * BLK : (n + 2) * BLK] = sb
            both = jnp.maximum(sa, sb)
            top = both if top is None else jnp.maximum(top, both)
        top = jnp.max(top, axis=1, keepdims=True) * factor
        tops[u] = jnp.maximum(jnp.broadcast_to(top, (BLK, width)), top_ref[step])

    def far_mix(step, u):
        i, h = row_block(step // heads), step % heads
        top = tops[u]
        scale = jnp.exp2(top_ref[step] - top)
        total, mixed = None, None
        for n in range(0, listed, 2):
            wa = jnp.exp2(scores[u][:, n * BLK : (n + 1) * BLK] * factor - top)
            wb = jnp.exp2(scores[u][:, (n + 1) * BLK : (n + 2) * BLK] * factor - top)
            total = wa + wb if total is None else total + (wa + wb)
            part = jnp.dot(
                jnp.concatenate([wa.astype(jnp.bfloat16), wb.astype(jnp.bfloat16)], axis=1),
                jnp.concatenate([far[found_s[h, n], 1], far[found_s[h, n + 1], 1]], axis=0),
                preferred_element_type=jnp.float32,
            )
            mixed = part if mixed is None else mixed + part
        total = jnp.sum(total, axis=1, keepdims=True) + total_ref[step] * scale
        mixed = mixed + mixed_ref[step] * scale
        rows = pl.ds(pl.multiple_of(i * BLK, BLK), BLK)
        staged[rows, pl.ds(pl.multiple_of(h * width, width), width)] = (mixed / total).astype(jnp.bfloat16)

    columns = pl.ds(pl.multiple_of(group * heads * width, heads * width), heads * width)

    def out_copy(k):
        i = row_block(k)
        owner, n = i // 2, k % 2
        return pltpu.make_async_remote_copy(
            staged.at[pl.ds(pl.multiple_of(i * BLK, BLK), BLK)],
            out_ref.at[pl.ds(pl.multiple_of(n * BLK, BLK), BLK), columns],
            out_send.at[k], out_recv.at[group * 2 + n],
            device_id=owner_of(owner), device_id_type=MESH,
        )

    def out_keep(k):
        i = row_block(k)
        n = k % 2
        return pltpu.make_async_copy(
            staged.at[pl.ds(pl.multiple_of(i * BLK, BLK), BLK)],
            out_ref.at[pl.ds(pl.multiple_of(n * BLK, BLK), BLK), columns],
            out_local.at[n],
        )

    def kept_here(k):
        return native & (row_block(k) // 2 == head)

    def out_in(of_group, n):
        return pltpu.make_async_remote_copy(
            staged.at[pl.ds(0, BLK)],
            out_ref.at[pl.ds(n * BLK, BLK), pl.ds(of_group * heads * width, heads * width)],
            out_send.at[0], out_recv.at[of_group * 2 + n],
            device_id=worker_of(jnp.int32(of_group)), device_id_type=MESH,
        )

    def send_block(k):
        @pl.when(kept_here(k))
        def _():
            out_keep(k).start()

        @pl.when(jnp.logical_not(kept_here(k)))
        def _():
            out_copy(k).start()

    def near_steps(k, j, carry):
        first = k * heads + 4 * j
        for u in range(4):
            near_scores(k, 4 * j + u, u)
            near_weigh(lax.rem(first + steps + u - 1, steps), (u + 3) % 4)
            near_mix(lax.rem(first + steps + u - 2, steps), (u + 2) % 4)
        return carry

    def near_group(ks):
        for k in ks:
            lax.fori_loop(0, heads // 4, functools.partial(near_steps, k), 0)
            for name in LATER[k] if k < len(LATER) else []:
                event(name)
        last = (ks[-1] + 1) * heads
        near_weigh(jnp.int32(last - 1), 3)
        for u in (2, 3):
            near_mix(jnp.int32(last - 4 + u), u)

    def far_group(ks):
        count, before = len(ks) * heads, ks[0] * heads

        def far_steps(j, carry):
            first = 4 * j
            for u in range(4):
                far_scores(before + lax.rem(first + u + 2, count), (u + 2) % 4)
                far_mix(before + first + u, u)

            @pl.when(j % 2 == 1)
            def _():
                send_block(ks[0] + j // 2)

            return carry

        for u in range(2):
            far_scores(jnp.int32(before + u), u)
        lax.fori_loop(0, count // 4, far_steps, 0)

    for k in range(blocks):
        wait_input(first_query + k)
    near_group(range(half))
    for name in NAMES:
        share(name, 1 - core).wait_recv()
    share("own", 1 - core).wait_recv()
    far_group(range(half))
    near_group(range(half, blocks))
    far_group(range(half, blocks))

    @pl.when(jnp.logical_not(native))
    def _():
        for k in range(len(sources)):
            swap(k).wait_send()

    for c in range(2):
        hop_one(c).wait_send()
        twin_one(c, True).wait_send()
        twin_two(c, True).wait_send()
    hop_two(1).wait_send()

    @pl.when(core == 1)
    def _():
        hop_two(0).wait_send()

    for name in NAMES:
        share(name, core).wait_send()
        if name != "zm3":
            send(name).wait_send()

    @pl.when(z == 1)
    def _():
        send("zm3").wait_send()

    share("own", core).wait_send()

    for k in range(blocks):

        @pl.when(kept_here(k))
        def _():
            out_keep(k).wait()

        @pl.when(jnp.logical_not(kept_here(k)))
        def _():
            out_copy(k).wait_send()

    for of_group in range(4):

        @pl.when(jnp.logical_not(native & (group == of_group)))
        def _():
            for n in range(2):
                out_in(of_group, n).wait_recv()


def shards(queries, keys, values, vertical, slash):
    width = keys.shape[1]
    rows = queries.shape[0]
    blocks = rows // BLK
    heads, listed = vertical.shape
    groups = lax.axis_size("head")
    kt = jnp.swapaxes(keys.reshape(blocks, BLK, width), 1, 2)
    v = values.reshape(blocks, BLK, width)
    dma = pltpu.SemaphoreType.DMA
    anywhere = pl.BlockSpec(memory_space=pl.ANY)
    bf16, f32 = jnp.bfloat16, jnp.float32
    inputs = 6 + blocks
    near_width = (listed + 1) * BLK
    return pl.pallas_call(
        functools.partial(layer_kernel, blocks=blocks, heads=heads, width=width, listed=listed),
        in_specs=[anywhere] * 5,
        out_specs=anywhere,
        out_shape=jax.ShapeDtypeStruct((rows // groups, groups * heads * width), bf16),
        scratch_shapes=[
            pltpu.VMEM((2, heads, listed), jnp.int32),
            pltpu.SMEM((2, heads, listed), jnp.int32),
            pltpu.VMEM((heads, listed), jnp.int32),
            pltpu.SMEM((heads, listed), jnp.int32),
            pltpu.SMEM((2, CAP), jnp.int32),
            pltpu.VMEM(queries.shape, bf16),
            pltpu.VMEM((blocks, 2, BLK, width), bf16),
            pltpu.VMEM((blocks, 2, BLK, width), bf16),
            pltpu.VMEM(((REACH + 1) * blocks, 2, BLK, width), bf16),
            pltpu.VMEM((2 * NODES * CAP, 2, BLK, width), bf16),
            pltpu.VMEM(queries.shape, bf16),
            pltpu.VMEM((heads * blocks, BLK, width), f32),
            pltpu.VMEM((heads * blocks, BLK, width), f32),
            pltpu.VMEM((heads * blocks, BLK, width), f32),
            pltpu.VMEM((BLK, near_width), f32),
            pltpu.VMEM((BLK, near_width), f32),
            pltpu.VMEM((BLK, near_width), f32),
            pltpu.VMEM((BLK, near_width), f32),
            pltpu.VMEM((BLK, near_width), bf16),
            pltpu.VMEM((BLK, near_width), bf16),
            pltpu.VMEM((BLK, near_width), bf16),
            pltpu.VMEM((BLK, near_width), bf16),
            pltpu.VMEM((4, BLK, width), f32),
            dma((inputs,)),
            dma((inputs,)),
            dma((inputs,)),
            dma((2,)),
            dma((8,)),
            dma((8,)),
            dma((len(NAMES),)),
            dma((len(NAMES),)),
            dma((len(NAMES) + 1,)),
            dma((len(NAMES) + 1,)),
            dma((2,)),
            dma((blocks,)),
            dma((2 * groups,)),
        ],
        compiler_params=pltpu.CompilerParams(
            collective_id=0, has_side_effects=True, vmem_limit_bytes=62 * 1024 * 1024
        ),
    )(slash, vertical, queries, kt, v)


def solution(mesh):
    in_specs = (
        P("seq", "head"),
        P("seq", "head"),
        P("seq", "head"),
        P("head", None),
        P("head", None),
    )
    out_specs = P(("seq", "head"), None)
    return jax.shard_map(shards, mesh=mesh, in_specs=in_specs, out_specs=out_specs, check_vma=False)
```

```python
import functools
import math

import jax
import jax.numpy as jnp
from jax import lax
from jax.experimental import pallas as pl
from jax.experimental.pallas import tpu as pltpu
from jax.sharding import PartitionSpec as P

BLK = 128
LARGEST_OFFSET = 28
CAP = 4
NEG = -1e30
SIDE = 4
NODES = SIDE * SIDE
REACH = 4
HALF = CAP // 2
MESH = pl.DeviceIdType.MESH

COPIES = {}
COPIES["zm"] = ((0, -1), (0, 0), "full")
COPIES["xp"] = ((1, 0), (0, 0), "full")
COPIES["xm"] = ((-1, 0), (0, 0), "full")
COPIES["zm2"] = ((0, -1), (0, 1), "full")
COPIES["zp"] = ((0, 1), (0, 0), "full")
COPIES["xm2"] = ((-1, 0), (1, 0), "full")
for d in (1, -1, 2):
    COPIES["xpA", d] = ((1, 0), (0, d), "A")
    COPIES["xmA", d] = ((-1, 0), (0, d), "A")
    COPIES["xmA2", d] = ((-1, 0), (1, d), "A")
    COPIES["zpB", d] = ((0, 1), (d, 0), "B")
    COPIES["zmB", d] = ((0, -1), (d, 0), "B")
    COPIES["zmB2", d] = ((0, -1), (d, 1), "B")
NAMES = list(COPIES)

THEN = {name: [] for name in NAMES}
THEN["zm"] = ["zm2", ("xpA", 1), ("xmA", 1)]
THEN["zm2"] = [("xpA", 2), ("xmA", 2)]
THEN["zp"] = [("xpA", -1), ("xmA", -1)]
THEN["xm"] = ["xm2", ("zmB", 1)]
THEN["xp"] = [("zmB", -1), ("zpB", -1)]
THEN["xm2"] = [("zmB", 2), ("zpB", 2)]
for d in (1, -1, 2):
    THEN["xmA", d] = [("xmA2", d)]
    THEN["zmB", d] = [("zmB2", d)]

FIRST = ["zm", "xm"]
SECOND = ["zm2", "xm2", ("zmB", 1), ("xmA", 1)]
LATER = [
    ["xp", "zp", ("xmA", 2), ("zmB", 2), ("zmB2", 1), ("xmA2", 1)],
    [("zmB", -1), ("xmA", -1), ("xmA2", 2), ("zmB2", 2)],
    [("xmA2", -1), ("zmB2", -1)],
    [(name, d) for d in (1, -1, 2) for name in ("xpA", "zpB")],
]


def layer_kernel(
    slash_ref,
    vertical_ref,
    queries_ref,
    kt_ref,
    v_ref,
    out_ref,
    table_v,
    table_s,
    found_v,
    found_s,
    picked_s,
    early_q,
    late_q,
    own_ref,
    hop_ref,
    near,
    far,
    staged,
    mixed_ref,
    top_ref,
    total_ref,
    scores_0,
    scores_1,
    scores_2,
    scores_3,
    weights_0,
    weights_1,
    weights_2,
    weights_3,
    tops,
    load_sem,
    swap_send,
    swap_recv,
    table_sem,
    near_send,
    near_recv,
    unit_send,
    unit_recv,
    twin_send,
    twin_recv,
    out_local,
    out_send,
    out_recv,
    *,
    blocks,
    heads,
    width,
    listed,
):
    seq, head = lax.axis_index("seq"), lax.axis_index("head")
    node, low = seq // 2, seq % 2
    high, core = head // 2, head % 2
    x, z = node // SIDE, node % SIDE
    group, slab = 2 * high + low, 2 * node + core
    native = low == core
    scores = (scores_0, scores_1, scores_2, scores_3)
    weights = (weights_0, weights_1, weights_2, weights_3)
    half = blocks // 2

    def at(dx, dz):
        to = lax.rem(x + dx + SIDE, SIDE) * SIDE + lax.rem(z + dz + SIDE, SIDE)
        return {"seq": 2 * to + low}

    follower = {"seq": 2 * lax.rem(node + 1, NODES) + low}
    leader = {"seq": 2 * lax.rem(node + NODES - 1, NODES) + low}
    twin = {"head": 2 * high + 1 - core}
    counterpart = {"seq": 2 * node + core, "head": 2 * high + low}

    def owner_of(quarter):
        return {"seq": slab, "head": quarter}

    def worker_of(of_group):
        return {"seq": 2 * node + lax.rem(of_group, 2), "head": 2 * (of_group // 2) + low}

    def row_block(k):
        late = k // half
        quarter = 2 * ((1 - late) * (1 - high) + late * high) + (k % half) // 2
        return 2 * quarter + k % 2

    sources = [slash_ref, vertical_ref]
    targets = [table_v.at[0], table_v.at[1]]
    for c in (1, 0):
        for kv, ref in enumerate((kt_ref, v_ref)):
            part = pl.ds(c * half, half)
            sources.append(ref.at[part])
            targets.append(own_ref.at[part, kv])
    first_query = len(sources)
    for k in range(blocks):
        rows = pl.ds(pl.multiple_of(row_block(k) * BLK, BLK), BLK)
        sources.append(queries_ref.at[rows])
        targets.append((early_q if k < half else late_q).at[pl.ds(k % half * BLK, BLK)])

    def load(k):
        return pltpu.make_async_copy(sources[k], targets[k], load_sem.at[k])

    def swap(k):
        return pltpu.make_async_remote_copy(
            sources[k], targets[k], swap_send.at[k], swap_recv.at[k],
            device_id=counterpart, device_id_type=MESH,
        )

    def wait_input(k):
        @pl.when(native)
        def _():
            load(k).wait()

        @pl.when(jnp.logical_not(native))
        def _():
            swap(k).wait_recv()

    def prepare(wait_table):
        for k in range(2):
            wait_table(k)
        to_scalars = pltpu.make_async_copy(table_v, table_s, table_sem.at[0])
        to_scalars.start()
        to_scalars.wait()

        def note_used(h, used):
            for n in range(listed):
                block = table_s[1, h, n] - (slab - 2) * blocks
                used = tuple(
                    u | (block == (j if j < blocks else j + blocks)).astype(jnp.int32)
                    for j, u in enumerate(used)
                )
            return used

        used = lax.fori_loop(0, heads, note_used, (jnp.int32(0),) * (2 * blocks))

        def choose(used):
            picked, rank = [jnp.int32(0)] * CAP, jnp.int32(0)
            for j in range(blocks):
                picked = [
                    jnp.where((used[j] == 1) & (rank == k), j, at_k) for k, at_k in enumerate(picked)
                ]
                rank = rank + used[j]
            return picked

        for c in range(2):
            for k, block in enumerate(choose(used[c * blocks : (c + 1) * blocks])):
                picked_s[c, k] = block

        verticals = table_v[1]
        first_of = verticals // blocks * blocks
        seen = jnp.zeros_like(verticals)
        for h in range(heads):
            for n in range(listed):
                there = table_s[1, h, n] - first_of
                for j in range(blocks - 1):
                    seen = seen | jnp.where(there == j, 1 << j, 0)
        before = verticals - first_of
        place = jnp.zeros_like(verticals)
        for j in range(blocks - 1):
            place = place + jnp.where((before > j) & (seen & (1 << j) != 0), 1, 0)
        of_slab = verticals // blocks
        found_v[...] = ((of_slab % 2) * NODES + of_slab // 2) * CAP + place
        to_found = pltpu.make_async_copy(found_v, found_s, table_sem.at[1])
        to_found.start()
        to_found.wait()

    @pl.when(native)
    def _():
        for k in range(len(sources)):
            load(k).start()

    barrier = pltpu.get_barrier_semaphore()

    def greet(device):
        pl.semaphore_signal(barrier, 1, device_id=device, device_id_type=MESH)

    for device in (at(1, 0), at(-1, 0), at(0, 1), at(0, -1), follower, leader, twin):
        greet(device)
    for k in range(4):

        @pl.when(jnp.logical_not(native & (head == k)))
        def _():
            greet(owner_of(k))

        @pl.when(jnp.logical_not(native & (group == k)))
        def _():
            greet(worker_of(jnp.int32(k)))

    @pl.when(jnp.logical_not(native))
    def _():
        greet(counterpart)

    @pl.when(native)
    def _():
        prepare(lambda k: load(k).wait())

    pl.semaphore_wait(barrier, 7 + 6 + 3 * (low - core) * (low - core))

    @pl.when(jnp.logical_not(native))
    def _():
        for k in range(len(sources)):
            swap(k).start()
        prepare(lambda k: swap(k).wait_recv())

    def near_copy(src, dst, k, device):
        return pltpu.make_async_remote_copy(
            src, dst, near_send.at[k], near_recv.at[k], device_id=device, device_id_type=MESH
        )

    def near_part(back, c):
        return near.at[pl.ds((REACH - back) * blocks + c * half, half)]

    def hop_one(c):
        part = pl.ds(c * half, half)
        return near_copy(own_ref.at[part], hop_ref.at[part], c, follower)

    def hop_two(c):
        return near_copy(hop_ref.at[pl.ds(c * half, half)], near_part(4, c), 2 + c, follower)

    def twin_one(c, from_own):
        src = (own_ref if from_own else hop_ref).at[pl.ds(c * half, half)]
        return near_copy(src, near_part(1, c), 4 + c, twin)

    def twin_two(c, from_hop):
        src = hop_ref.at[pl.ds(c * half, half)] if from_hop else near_part(4, c)
        return near_copy(src, near_part(3, c), 6 + c, twin)

    def unit(dx, dz, part, of_core):
        to = lax.rem(x + dx + SIDE, SIDE) * SIDE + lax.rem(z + dz + SIDE, SIDE)
        first = (of_core * NODES + to) * CAP
        if part == "full":
            return far.at[pl.ds(pl.multiple_of(first, CAP), CAP)]
        if part == "B":
            first = first + HALF
        return far.at[pl.ds(pl.multiple_of(first, HALF), HALF)]

    def arrives(name):
        (sx, sz), (dx, dz), part = COPIES[name]
        return dx - sx, dz - sz, part

    def send(name):
        (sx, sz), (dx, dz), part = COPIES[name]
        ref, k = unit(dx, dz, part, core), NAMES.index(name)
        return pltpu.make_async_remote_copy(
            ref, ref, unit_send.at[k], unit_recv.at[k], device_id=at(sx, sz), device_id_type=MESH
        )

    def receive(name):
        (sx, sz), _, _ = COPIES[name]
        ref, k = unit(*arrives(name), core), NAMES.index(name)
        return pltpu.make_async_remote_copy(
            ref, ref, unit_send.at[k], unit_recv.at[k], device_id=at(-sx, -sz), device_id_type=MESH
        )

    def share(name, of_core):
        ref = unit(0, 0, "full", of_core) if name == "own" else unit(*arrives(name), of_core)
        k = len(NAMES) if name == "own" else NAMES.index(name)
        return pltpu.make_async_remote_copy(
            ref, ref, twin_send.at[k], twin_recv.at[k], device_id=twin, device_id_type=MESH
        )

    def start(name):
        if name[0] == "zpB":
            return
        if name == "xp" or name[0] == "xpA":

            @pl.when(z < SIDE - 1)
            def _():
                send(name).start()

        else:
            send(name).start()

    def event(name):
        receive(name).wait_recv()
        for following in THEN[name]:
            start(following)
        share(name, core).start()

    def pack(src, node_of, c):
        first = pl.multiple_of((core * NODES + node_of) * CAP, CAP)
        for k in range(CAP):
            for kv in range(2):
                far[first + k, kv] = src[picked_s[c, k], kv]

    for c in (1, 0):
        for k in range(2):
            wait_input(2 + 2 * (1 - c) + k)
        hop_one(c).start()

        @pl.when(core == 0)
        def _():
            twin_one(c, True).start()

    pack(own_ref, node, 1)
    for j in range(blocks):
        for kv in range(2):
            near[REACH * blocks + j, kv] = own_ref[j, kv]
    for name in ("zm", "xm", "xp"):
        start(name)
    share("own", core).start()

    for name in FIRST:
        event(name)
    for c in (1, 0):
        hop_one(c).wait_recv()
        if c == 1:
            hop_two(c).start()
        else:

            @pl.when(core == 1)
            def _():
                hop_two(c).start()

        @pl.when(core == 1)
        def _():
            twin_one(c, False).start()

        @pl.when(core == 0)
        def _():
            twin_two(c, True).start()

    @pl.when(z > 0)
    def _():
        pack(hop_ref, x * SIDE + z - 1, 0)

    for j in range(blocks):
        for kv in range(2):
            near[2 * blocks + j, kv] = hop_ref[j, kv]

    @pl.when(z > 0)
    def _():
        for following in THEN["zp"]:
            start(following)
        share("zp", core).start()

    @pl.when(z == SIDE - 1)
    def _():
        send("zp").start()
        send("xp").start()

    @pl.when(z < SIDE - 1)
    def _():
        event("xp")

    for name in SECOND:
        event(name)

    @pl.when(core == 1)
    def _():
        for c in (1, 0):
            hop_two(c).wait_recv()
            twin_two(c, False).start()

    @pl.when(core == 0)
    def _():
        hop_two(1).wait_recv()

    for c in range(2):
        twin_one(c, True).wait_recv()
        twin_two(c, True).wait_recv()

    for d in (1, 2):
        send(("zpB", d)).start()

    @pl.when(z < SIDE - 1)
    def _():
        send(("zpB", -1)).start()

    @pl.when(z == SIDE - 1)
    def _():
        for d in (1, -1, 2):
            send(("xpA", d)).start()

    factor = math.log2(math.e) / math.sqrt(width)
    causal = lax.broadcasted_iota(jnp.int32, (BLK, BLK), 0) >= lax.broadcasted_iota(
        jnp.int32, (BLK, BLK), 1
    )
    kept = heads * half
    base = slab * blocks

    def query(ref, k, h):
        return ref[
            pl.ds(pl.multiple_of(k % half * BLK, BLK), BLK),
            pl.ds(pl.multiple_of(h * width, width), width),
        ]

    def pair_scores(q, ref, a, b, bias_a, bias_b):
        pair = jnp.dot(
            q, jnp.concatenate([ref[a, 0], ref[b, 0]], axis=1), preferred_element_type=jnp.float32
        )
        return pair[:, :BLK] + bias_a, pair[:, BLK:] + bias_b

    def pair_mix(u, n, ref, a, b):
        return jnp.dot(
            weights[u][:, n * BLK : (n + 2) * BLK],
            jnp.concatenate([ref[a, 1], ref[b, 1]], axis=0),
            preferred_element_type=jnp.float32,
        )

    def row_top(u, count):
        top = scores[u][:, :BLK]
        for n in range(1, count):
            top = jnp.maximum(top, scores[u][:, n * BLK : (n + 1) * BLK])
        return jnp.broadcast_to(jnp.max(top, axis=1, keepdims=True) * factor, (BLK, width))

    def weigh(u, count, top):
        total = None
        for n in range(count):
            w = jnp.exp2(scores[u][:, n * BLK : (n + 1) * BLK] * factor - top)
            total = w if total is None else total + w
            weights[u][:, n * BLK : (n + 1) * BLK] = w.astype(jnp.bfloat16)
        return jnp.broadcast_to(jnp.sum(total, axis=1, keepdims=True), (BLK, width))

    def near_entry(i, h, n):
        offset = table_s[0, h, n]
        return REACH * blocks + i - offset, jnp.where(base + i >= offset, 0.0, NEG)

    def near_scores(k, h, u):
        i = row_block(k)
        q = query(early_q, k, h)
        own = jnp.dot(q, near[REACH * blocks + i, 0], preferred_element_type=jnp.float32)
        scores[u][:, :BLK] = jnp.where(causal, own, NEG)
        for n in range(0, listed, 2):
            (a, bias_a), (b, bias_b) = near_entry(i, h, n), near_entry(i, h, n + 1)
            sa, sb = pair_scores(q, near, a, b, bias_a, bias_b)
            scores[u][:, (n + 1) * BLK : (n + 2) * BLK] = sa
            scores[u][:, (n + 2) * BLK : (n + 3) * BLK] = sb

    def near_weigh(step, u):
        top_ref[step] = row_top(u, listed + 1)
        total_ref[step] = weigh(u, listed + 1, top_ref[step])

    def near_mix(step, u):
        i, h = row_block(step // heads), step % heads
        mixed = jnp.dot(
            weights[u][:, :BLK], near[REACH * blocks + i, 1], preferred_element_type=jnp.float32
        )
        for n in range(0, listed, 2):
            a, b = near_entry(i, h, n)[0], near_entry(i, h, n + 1)[0]
            mixed = mixed + pair_mix(u, n + 1, near, a, b)
        mixed_ref[step] = mixed

    def far_bias(own, h, block):
        gap = own - block
        ok = gap > 0
        for n in range(listed):
            ok = ok & (gap != table_s[0, h, n])
        return jnp.where(ok, 0.0, NEG)

    def far_scores(step, u):
        i, h = row_block(step // heads), step % heads
        q = query(early_q, step // heads, h)
        top = None
        for n in range(0, listed, 2):
            bias = [far_bias(base + i, h, table_s[1, h, n + d]) for d in range(2)]
            sa, sb = pair_scores(q, far, found_s[h, n], found_s[h, n + 1], *bias)
            scores[u][:, n * BLK : (n + 1) * BLK] = sa
            scores[u][:, (n + 1) * BLK : (n + 2) * BLK] = sb
            both = jnp.maximum(sa, sb)
            top = both if top is None else jnp.maximum(top, both)
        top = jnp.max(top, axis=1, keepdims=True) * factor
        tops[u] = jnp.maximum(jnp.broadcast_to(top, (BLK, width)), top_ref[step])

    def far_mix(step, u):
        i, h = row_block(step // heads), step % heads
        top = tops[u]
        scale = jnp.exp2(top_ref[step] - top)
        total, mixed = None, None
        for n in range(0, listed, 2):
            wa = jnp.exp2(scores[u][:, n * BLK : (n + 1) * BLK] * factor - top)
            wb = jnp.exp2(scores[u][:, (n + 1) * BLK : (n + 2) * BLK] * factor - top)
            total = wa + wb if total is None else total + (wa + wb)
            part = jnp.dot(
                jnp.concatenate([wa.astype(jnp.bfloat16), wb.astype(jnp.bfloat16)], axis=1),
                jnp.concatenate([far[found_s[h, n], 1], far[found_s[h, n + 1], 1]], axis=0),
                preferred_element_type=jnp.float32,
            )
            mixed = part if mixed is None else mixed + part
        total = jnp.sum(total, axis=1, keepdims=True) + total_ref[step] * scale
        mixed = mixed + mixed_ref[step] * scale
        rows = pl.ds(pl.multiple_of(i * BLK, BLK), BLK)
        staged[rows, pl.ds(pl.multiple_of(h * width, width), width)] = (mixed / total).astype(jnp.bfloat16)

    part = heads * width // 2

    def out_refs(k, c):
        i = row_block(k)
        here = staged.at[
            pl.ds(pl.multiple_of(i * BLK, BLK), BLK), pl.ds(pl.multiple_of(c * part, part), part)
        ]
        first = pl.multiple_of((group * 2 + c) * part, part)
        return here, out_ref.at[pl.ds(pl.multiple_of(k % 2 * BLK, BLK), BLK), pl.ds(first, part)]

    def out_copy(k, c):
        here, there = out_refs(k, c)
        return pltpu.make_async_remote_copy(
            here, there, out_send.at[k * 2 + c], out_recv.at[group * 4 + k % 2 * 2 + c],
            device_id=owner_of(row_block(k) // 2), device_id_type=MESH,
        )

    def out_keep(k, c):
        here, there = out_refs(k, c)
        return pltpu.make_async_copy(here, there, out_local.at[k % 2 * 2 + c])

    def kept_here(k):
        return native & (row_block(k) // 2 == head)

    def out_in(of_group, n, c):
        return pltpu.make_async_remote_copy(
            staged.at[pl.ds(0, BLK), pl.ds(0, part)],
            out_ref.at[pl.ds(n * BLK, BLK), pl.ds((of_group * 2 + c) * part, part)],
            out_send.at[0], out_recv.at[of_group * 4 + n * 2 + c],
            device_id=worker_of(jnp.int32(of_group)), device_id_type=MESH,
        )

    def send_part(k, c):
        @pl.when(kept_here(k))
        def _():
            out_keep(k, c).start()

        @pl.when(jnp.logical_not(kept_here(k)))
        def _():
            out_copy(k, c).start()

    def near_steps(k, j, carry):
        first = k * heads + 4 * j
        for u in range(4):
            near_scores(k, 4 * j + u, u)
            near_weigh(lax.rem(first + kept + u - 1, kept), (u + 3) % 4)
            near_mix(lax.rem(first + kept + u - 2, kept), (u + 2) % 4)
        return carry

    def near_group(ks):
        for k in ks:
            lax.fori_loop(0, heads // 4, functools.partial(near_steps, k), 0)
            for name in LATER[k] if k < len(LATER) else []:
                if name == "xp":

                    @pl.when(z == SIDE - 1)
                    def _():
                        event("xp")
                        send(("zpB", -1)).start()

                elif name == "zp":

                    @pl.when(z == 0)
                    def _():
                        event("zp")

                else:
                    event(name)
        last = (ks[-1] + 1) * heads
        near_weigh(jnp.int32(last - 1), 3)
        for u in (2, 3):
            near_mix(jnp.int32(last - 4 + u), u)

    def far_group(ks):
        count, before = len(ks) * heads, ks[0] * heads

        def far_steps(j, carry):
            first = 4 * j
            for u in range(4):
                far_scores(before + lax.rem(first + u + 2, count), (u + 2) % 4)
                far_mix(before + first + u, u)

            send_part(ks[0] + j // 2, j % 2)
            return carry

        for u in range(2):
            far_scores(jnp.int32(before + u), u)
        lax.fori_loop(0, count // 4, far_steps, 0)

    def full_scores(step, u):
        k, h = step // heads, step % heads
        i = row_block(k)
        q = query(late_q, k, h)
        own = jnp.dot(q, near[REACH * blocks + i, 0], preferred_element_type=jnp.float32)
        own = jnp.where(causal, own, NEG)
        scores[u][:, :BLK] = own
        top = own
        for n in range(0, 2 * listed, 2):
            if n < listed:
                ref = near
                (a, bias_a), (b, bias_b) = near_entry(i, h, n), near_entry(i, h, n + 1)
            else:
                ref, m = far, n - listed
                a, b = found_s[h, m], found_s[h, m + 1]
                bias_a, bias_b = (far_bias(base + i, h, table_s[1, h, m + d]) for d in range(2))
            sa, sb = pair_scores(q, ref, a, b, bias_a, bias_b)
            scores[u][:, (n + 1) * BLK : (n + 2) * BLK] = sa
            scores[u][:, (n + 2) * BLK : (n + 3) * BLK] = sb
            top = jnp.maximum(top, jnp.maximum(sa, sb))
        tops[u] = jnp.broadcast_to(jnp.max(top, axis=1, keepdims=True) * factor, (BLK, width))

    def full_mix(step, u):
        i, h = row_block(step // heads), step % heads
        top = tops[u]

        def weight(n):
            return jnp.exp2(scores[u][:, n * BLK : (n + 1) * BLK] * factor - top)

        total = weight(0)
        mixed = jnp.dot(
            total.astype(jnp.bfloat16), near[REACH * blocks + i, 1], preferred_element_type=jnp.float32
        )
        for n in range(0, 2 * listed, 2):
            if n < listed:
                ref, a, b = near, near_entry(i, h, n)[0], near_entry(i, h, n + 1)[0]
            else:
                ref, a, b = far, found_s[h, n - listed], found_s[h, n - listed + 1]
            wa, wb = weight(n + 1), weight(n + 2)
            total = total + (wa + wb)
            mixed = mixed + jnp.dot(
                jnp.concatenate([wa.astype(jnp.bfloat16), wb.astype(jnp.bfloat16)], axis=1),
                jnp.concatenate([ref[a, 1], ref[b, 1]], axis=0),
                preferred_element_type=jnp.float32,
            )
        total = jnp.sum(total, axis=1, keepdims=True)
        rows = pl.ds(pl.multiple_of(i * BLK, BLK), BLK)
        staged[rows, pl.ds(pl.multiple_of(h * width, width), width)] = (mixed / total).astype(jnp.bfloat16)

    def full_group(ks):
        count, before = len(ks) * heads, ks[0] * heads

        def full_steps(j, carry):
            first = 4 * j
            for u in range(4):
                full_scores(before + lax.rem(first + u + 2, count), (u + 2) % 4)
                full_mix(before + first + u, u)
            send_part(ks[0] + j // 2, j % 2)
            return carry

        for u in range(2):
            full_scores(jnp.int32(before + u), u)
        lax.fori_loop(0, count // 4, full_steps, 0)

    for k in range(half):
        wait_input(first_query + k)
    near_group(range(half))
    for name in NAMES:
        share(name, 1 - core).wait_recv()
    share("own", 1 - core).wait_recv()
    far_group(range(half))
    for k in range(half, blocks):
        wait_input(first_query + k)
    full_group(range(half, blocks))

    @pl.when(jnp.logical_not(native))
    def _():
        for k in range(len(sources)):
            swap(k).wait_send()

    for c in range(2):
        hop_one(c).wait_send()
        twin_one(c, True).wait_send()
        twin_two(c, True).wait_send()
    hop_two(1).wait_send()

    @pl.when(core == 1)
    def _():
        hop_two(0).wait_send()

    for name in NAMES:
        share(name, core).wait_send()
        if name != "zp":
            send(name).wait_send()

    @pl.when(z == SIDE - 1)
    def _():
        send("zp").wait_send()

    share("own", core).wait_send()

    for k in range(blocks):

        @pl.when(kept_here(k))
        def _():
            for c in range(2):
                out_keep(k, c).wait()

        @pl.when(jnp.logical_not(kept_here(k)))
        def _():
            for c in range(2):
                out_copy(k, c).wait_send()

    for of_group in range(4):

        @pl.when(jnp.logical_not(native & (group == of_group)))
        def _():
            for n in range(2):
                for c in range(2):
                    out_in(of_group, n, c).wait_recv()


def shards(queries, keys, values, vertical, slash):
    width = keys.shape[1]
    rows = queries.shape[0]
    blocks = rows // BLK
    heads, listed = vertical.shape
    groups = lax.axis_size("head")
    kt = jnp.swapaxes(keys.reshape(blocks, BLK, width), 1, 2)
    v = values.reshape(blocks, BLK, width)
    dma = pltpu.SemaphoreType.DMA
    anywhere = pl.BlockSpec(memory_space=pl.ANY)
    bf16, f32 = jnp.bfloat16, jnp.float32
    inputs = 6 + blocks
    full_width = (2 * listed + 1) * BLK
    return pl.pallas_call(
        functools.partial(layer_kernel, blocks=blocks, heads=heads, width=width, listed=listed),
        in_specs=[anywhere] * 5,
        out_specs=anywhere,
        out_shape=jax.ShapeDtypeStruct((rows // groups, groups * heads * width), bf16),
        scratch_shapes=[
            pltpu.VMEM((2, heads, listed), jnp.int32),
            pltpu.SMEM((2, heads, listed), jnp.int32),
            pltpu.VMEM((heads, listed), jnp.int32),
            pltpu.SMEM((heads, listed), jnp.int32),
            pltpu.SMEM((2, CAP), jnp.int32),
            pltpu.VMEM((rows // 2, heads * width), bf16),
            pltpu.VMEM((rows // 2, heads * width), bf16),
            pltpu.VMEM((blocks, 2, BLK, width), bf16),
            pltpu.VMEM((blocks, 2, BLK, width), bf16),
            pltpu.VMEM(((REACH + 1) * blocks, 2, BLK, width), bf16),
            pltpu.VMEM((2 * NODES * CAP, 2, BLK, width), bf16),
            pltpu.VMEM(queries.shape, bf16),
            pltpu.VMEM((heads * blocks // 2, BLK, width), f32),
            pltpu.VMEM((heads * blocks // 2, BLK, width), f32),
            pltpu.VMEM((heads * blocks // 2, BLK, width), f32),
            pltpu.VMEM((BLK, full_width), f32),
            pltpu.VMEM((BLK, full_width), f32),
            pltpu.VMEM((BLK, full_width), f32),
            pltpu.VMEM((BLK, full_width), f32),
            pltpu.VMEM((BLK, full_width), bf16),
            pltpu.VMEM((BLK, full_width), bf16),
            pltpu.VMEM((BLK, full_width), bf16),
            pltpu.VMEM((BLK, full_width), bf16),
            pltpu.VMEM((4, BLK, width), f32),
            dma((inputs,)),
            dma((inputs,)),
            dma((inputs,)),
            dma((2,)),
            dma((8,)),
            dma((8,)),
            dma((len(NAMES),)),
            dma((len(NAMES),)),
            dma((len(NAMES) + 1,)),
            dma((len(NAMES) + 1,)),
            dma((4,)),
            dma((2 * blocks,)),
            dma((4 * groups,)),
        ],
        compiler_params=pltpu.CompilerParams(
            collective_id=0, has_side_effects=True, vmem_limit_bytes=62 * 1024 * 1024
        ),
    )(slash, vertical, queries, kt, v)


def solution(mesh):
    in_specs = (
        P("seq", "head"),
        P("seq", "head"),
        P("seq", "head"),
        P("head", None),
        P("head", None),
    )
    out_specs = P(("seq", "head"), None)
    return jax.shard_map(shards, mesh=mesh, in_specs=in_specs, out_specs=out_specs, check_vma=False)
```

```python
import functools
import math

import jax
import jax.numpy as jnp
from jax import lax
from jax.experimental import pallas as pl
from jax.experimental.pallas import tpu as pltpu
from jax.sharding import PartitionSpec as P

BLK = 128
LARGEST_OFFSET = 28
CAP = 4
NEG = -1e30
SIDE = 4
NODES = SIDE * SIDE
REACH = 4
HALF = CAP // 2
EARLY = 6
MESH = pl.DeviceIdType.MESH

COPIES = {}
COPIES["zm"] = ((0, -1), (0, 0), "full")
COPIES["xp"] = ((1, 0), (0, 0), "full")
COPIES["xm"] = ((-1, 0), (0, 0), "full")
COPIES["zm2"] = ((0, -1), (0, 1), "full")
COPIES["zp"] = ((0, 1), (0, 0), "full")
COPIES["xm2"] = ((-1, 0), (1, 0), "full")
for d in (1, -1, 2):
    COPIES["xpA", d] = ((1, 0), (0, d), "A")
    COPIES["xmA", d] = ((-1, 0), (0, d), "A")
    COPIES["xmA2", d] = ((-1, 0), (1, d), "A")
    COPIES["zpB", d] = ((0, 1), (d, 0), "B")
    COPIES["zmB", d] = ((0, -1), (d, 0), "B")
    COPIES["zmB2", d] = ((0, -1), (d, 1), "B")
NAMES = list(COPIES)

THEN = {name: [] for name in NAMES}
THEN["zm"] = ["zm2", ("xpA", 1), ("xmA", 1)]
THEN["zm2"] = [("xpA", 2), ("xmA", 2)]
THEN["zp"] = [("xpA", -1), ("xmA", -1)]
THEN["xm"] = ["xm2", ("zmB", 1)]
THEN["xp"] = [("zmB", -1), ("zpB", -1)]
THEN["xm2"] = [("zmB", 2), ("zpB", 2)]
for d in (1, -1, 2):
    THEN["xmA", d] = [("xmA2", d)]
    THEN["zmB", d] = [("zmB2", d)]

FIRST = ["zm", "xm"]
SECOND = ["zm2", "xm2", ("zmB", 1), ("xmA", 1)]
LATER = [
    ["xp", "zp", ("xmA", 2), ("zmB", 2), ("zmB2", 1), ("xmA2", 1)],
    [("zmB", -1)],
    [("xmA", -1)],
    [("zmB2", 2), ("xmA2", 2)],
    [("xmA2", -1), ("zmB2", -1)],
    [(name, d) for d in (1, -1, 2) for name in ("xpA", "zpB")],
]


def layer_kernel(
    slash_ref,
    vertical_ref,
    queries_ref,
    k_ref,
    v_ref,
    out_ref,
    table_v,
    table_s,
    found_v,
    found_s,
    picked_s,
    early_q,
    late_q,
    keys_v,
    own_ref,
    hop_ref,
    near,
    far,
    staged,
    mixed_ref,
    top_ref,
    total_ref,
    scores_0,
    scores_1,
    scores_2,
    scores_3,
    weights_0,
    weights_1,
    weights_2,
    weights_3,
    tops,
    load_sem,
    swap_send,
    swap_recv,
    table_sem,
    near_send,
    near_recv,
    unit_send,
    unit_recv,
    twin_send,
    twin_recv,
    out_local,
    out_send,
    out_recv,
    *,
    blocks,
    heads,
    width,
    listed,
):
    seq, head = lax.axis_index("seq"), lax.axis_index("head")
    node, low = seq // 2, seq % 2
    high, core = head // 2, head % 2
    x, z = node // SIDE, node % SIDE
    group, slab = 2 * high + low, 2 * node + core
    native = low == core
    scores = (scores_0, scores_1, scores_2, scores_3)
    weights = (weights_0, weights_1, weights_2, weights_3)
    half = blocks // 2

    def at(dx, dz):
        to = lax.rem(x + dx + SIDE, SIDE) * SIDE + lax.rem(z + dz + SIDE, SIDE)
        return {"seq": 2 * to + low}

    follower = {"seq": 2 * lax.rem(node + 1, NODES) + low}
    leader = {"seq": 2 * lax.rem(node + NODES - 1, NODES) + low}
    twin = {"head": 2 * high + 1 - core}
    counterpart = {"seq": 2 * node + core, "head": 2 * high + low}

    def owner_of(quarter):
        return {"seq": slab, "head": quarter}

    def worker_of(of_group):
        return {"seq": 2 * node + lax.rem(of_group, 2), "head": 2 * (of_group // 2) + low}

    def row_block(k):
        late = k // half
        quarter = 2 * ((1 - late) * (1 - high) + late * high) + (k % half) // 2
        return 2 * quarter + k % 2

    sources = [slash_ref, vertical_ref]
    targets = [table_v.at[0], table_v.at[1]]
    for c in (1, 0):
        part = pl.ds(c * half, half)
        sources += [k_ref.at[part], v_ref.at[part]]
        targets += [keys_v.at[part], own_ref.at[part, 1]]
    first_query = len(sources)
    for k in range(blocks):
        rows = pl.ds(pl.multiple_of(row_block(k) * BLK, BLK), BLK)
        sources.append(queries_ref.at[rows])
        ref, place = (early_q, k) if k < EARLY else (late_q, k - EARLY)
        targets.append(ref.at[pl.ds(place * BLK, BLK)])

    def load(k):
        return pltpu.make_async_copy(sources[k], targets[k], load_sem.at[k])

    def swap(k):
        return pltpu.make_async_remote_copy(
            sources[k], targets[k], swap_send.at[k], swap_recv.at[k],
            device_id=counterpart, device_id_type=MESH,
        )

    def wait_input(k):
        @pl.when(native)
        def _():
            load(k).wait()

        @pl.when(jnp.logical_not(native))
        def _():
            swap(k).wait_recv()

    def prepare(wait_table):
        for k in range(2):
            wait_table(k)
        to_scalars = pltpu.make_async_copy(table_v, table_s, table_sem.at[0])
        to_scalars.start()
        to_scalars.wait()

        def note_used(h, used):
            for n in range(listed):
                block = table_s[1, h, n] - (slab - 2) * blocks
                used = tuple(
                    u | (block == (j if j < blocks else j + blocks)).astype(jnp.int32)
                    for j, u in enumerate(used)
                )
            return used

        used = lax.fori_loop(0, heads, note_used, (jnp.int32(0),) * (2 * blocks))

        def choose(used):
            picked, rank = [jnp.int32(0)] * CAP, jnp.int32(0)
            for j in range(blocks):
                picked = [
                    jnp.where((used[j] == 1) & (rank == k), j, at_k) for k, at_k in enumerate(picked)
                ]
                rank = rank + used[j]
            return picked

        for c in range(2):
            for k, block in enumerate(choose(used[c * blocks : (c + 1) * blocks])):
                picked_s[c, k] = block

        verticals = table_v[1]
        first_of = verticals // blocks * blocks
        seen = jnp.zeros_like(verticals)
        for h in range(heads):
            for n in range(listed):
                there = table_s[1, h, n] - first_of
                for j in range(blocks - 1):
                    seen = seen | jnp.where(there == j, 1 << j, 0)
        before = verticals - first_of
        place = jnp.zeros_like(verticals)
        for j in range(blocks - 1):
            place = place + jnp.where((before > j) & (seen & (1 << j) != 0), 1, 0)
        of_slab = verticals // blocks
        found_v[...] = ((of_slab % 2) * NODES + of_slab // 2) * CAP + place
        to_found = pltpu.make_async_copy(found_v, found_s, table_sem.at[1])
        to_found.start()
        to_found.wait()

    @pl.when(native)
    def _():
        for k in range(len(sources)):
            load(k).start()

    barrier = pltpu.get_barrier_semaphore()

    def greet(device):
        pl.semaphore_signal(barrier, 1, device_id=device, device_id_type=MESH)

    for device in (at(1, 0), at(-1, 0), at(0, 1), at(0, -1), follower, leader, twin):
        greet(device)
    for k in range(4):

        @pl.when(jnp.logical_not(native & (head == k)))
        def _():
            greet(owner_of(k))

        @pl.when(jnp.logical_not(native & (group == k)))
        def _():
            greet(worker_of(jnp.int32(k)))

    @pl.when(jnp.logical_not(native))
    def _():
        greet(counterpart)

    @pl.when(native)
    def _():
        prepare(lambda k: load(k).wait())

    pl.semaphore_wait(barrier, 7 + 6 + 3 * (low - core) * (low - core))

    @pl.when(jnp.logical_not(native))
    def _():
        for k in range(len(sources)):
            swap(k).start()
        prepare(lambda k: swap(k).wait_recv())

    def near_copy(src, dst, k, device):
        return pltpu.make_async_remote_copy(
            src, dst, near_send.at[k], near_recv.at[k], device_id=device, device_id_type=MESH
        )

    def near_part(back, c):
        return near.at[pl.ds((REACH - back) * blocks + c * half, half)]

    def hop_one(c):
        part = pl.ds(c * half, half)
        return near_copy(own_ref.at[part], hop_ref.at[part], c, follower)

    def hop_two(c):
        return near_copy(hop_ref.at[pl.ds(c * half, half)], near_part(4, c), 2 + c, follower)

    def twin_one(c, from_own):
        src = (own_ref if from_own else hop_ref).at[pl.ds(c * half, half)]
        return near_copy(src, near_part(1, c), 4 + c, twin)

    def twin_two(c, from_hop):
        src = hop_ref.at[pl.ds(c * half, half)] if from_hop else near_part(4, c)
        return near_copy(src, near_part(3, c), 6 + c, twin)

    def unit(dx, dz, part, of_core):
        to = lax.rem(x + dx + SIDE, SIDE) * SIDE + lax.rem(z + dz + SIDE, SIDE)
        first = (of_core * NODES + to) * CAP
        if part == "full":
            return far.at[pl.ds(pl.multiple_of(first, CAP), CAP)]
        if part == "B":
            first = first + HALF
        return far.at[pl.ds(pl.multiple_of(first, HALF), HALF)]

    def arrives(name):
        (sx, sz), (dx, dz), part = COPIES[name]
        return dx - sx, dz - sz, part

    def send(name):
        (sx, sz), (dx, dz), part = COPIES[name]
        ref, k = unit(dx, dz, part, core), NAMES.index(name)
        return pltpu.make_async_remote_copy(
            ref, ref, unit_send.at[k], unit_recv.at[k], device_id=at(sx, sz), device_id_type=MESH
        )

    def receive(name):
        (sx, sz), _, _ = COPIES[name]
        ref, k = unit(*arrives(name), core), NAMES.index(name)
        return pltpu.make_async_remote_copy(
            ref, ref, unit_send.at[k], unit_recv.at[k], device_id=at(-sx, -sz), device_id_type=MESH
        )

    def share(name, of_core):
        ref = unit(0, 0, "full", of_core) if name == "own" else unit(*arrives(name), of_core)
        k = len(NAMES) if name == "own" else NAMES.index(name)
        return pltpu.make_async_remote_copy(
            ref, ref, twin_send.at[k], twin_recv.at[k], device_id=twin, device_id_type=MESH
        )

    def start(name):
        if name[0] == "zpB":
            return
        if name == "xp" or name[0] == "xpA":

            @pl.when(z < SIDE - 1)
            def _():
                send(name).start()

        else:
            send(name).start()

    def event(name):
        receive(name).wait_recv()
        for following in THEN[name]:
            start(following)
        share(name, core).start()

    def pack(src, node_of, c):
        first = pl.multiple_of((core * NODES + node_of) * CAP, CAP)
        for k in range(CAP):
            for kv in range(2):
                far[first + k, kv] = src[picked_s[c, k], kv]

    for c in (1, 0):
        for k in range(2):
            wait_input(2 + 2 * (1 - c) + k)
        for j in range(c * half, (c + 1) * half):
            own_ref[j, 0] = keys_v[j].T
        hop_one(c).start()

        @pl.when(core == 0)
        def _():
            twin_one(c, True).start()

    pack(own_ref, node, 1)
    for j in range(blocks):
        for kv in range(2):
            near[REACH * blocks + j, kv] = own_ref[j, kv]
    for name in ("zm", "xm", "xp"):
        start(name)
    share("own", core).start()

    for name in FIRST:
        event(name)
    for c in (1, 0):
        hop_one(c).wait_recv()
        if c == 1:
            hop_two(c).start()
        else:

            @pl.when(core == 1)
            def _():
                hop_two(c).start()

        @pl.when(core == 1)
        def _():
            twin_one(c, False).start()

        @pl.when(core == 0)
        def _():
            twin_two(c, True).start()

    @pl.when(z > 0)
    def _():
        pack(hop_ref, x * SIDE + z - 1, 0)

    for j in range(blocks):
        for kv in range(2):
            near[2 * blocks + j, kv] = hop_ref[j, kv]

    @pl.when(z > 0)
    def _():
        for following in THEN["zp"]:
            start(following)
        share("zp", core).start()

    @pl.when(z == SIDE - 1)
    def _():
        send("zp").start()
        send("xp").start()

    @pl.when(z < SIDE - 1)
    def _():
        event("xp")

    for name in SECOND:
        event(name)

    @pl.when(core == 1)
    def _():
        for c in (1, 0):
            hop_two(c).wait_recv()
            twin_two(c, False).start()

    @pl.when(core == 0)
    def _():
        hop_two(1).wait_recv()

    for c in range(2):
        twin_one(c, True).wait_recv()
        twin_two(c, True).wait_recv()

    for d in (1, 2):
        send(("zpB", d)).start()

    @pl.when(z < SIDE - 1)
    def _():
        send(("zpB", -1)).start()

    @pl.when(z == SIDE - 1)
    def _():
        for d in (1, -1, 2):
            send(("xpA", d)).start()

    factor = math.log2(math.e) / math.sqrt(width)
    causal = lax.broadcasted_iota(jnp.int32, (BLK, BLK), 0) >= lax.broadcasted_iota(
        jnp.int32, (BLK, BLK), 1
    )
    kept = heads * EARLY
    base = slab * blocks

    def query(ref, k, h):
        return ref[
            pl.ds(pl.multiple_of(k * BLK, BLK), BLK),
            pl.ds(pl.multiple_of(h * width, width), width),
        ]

    def pair_scores(q, ref, a, b, bias_a, bias_b):
        pair = jnp.dot(
            q, jnp.concatenate([ref[a, 0], ref[b, 0]], axis=1), preferred_element_type=jnp.float32
        )
        return pair[:, :BLK] + bias_a, pair[:, BLK:] + bias_b

    def pair_mix(u, n, ref, a, b):
        return jnp.dot(
            weights[u][:, n * BLK : (n + 2) * BLK],
            jnp.concatenate([ref[a, 1], ref[b, 1]], axis=0),
            preferred_element_type=jnp.float32,
        )

    def row_top(u, count):
        top = scores[u][:, :BLK]
        for n in range(1, count):
            top = jnp.maximum(top, scores[u][:, n * BLK : (n + 1) * BLK])
        return jnp.broadcast_to(jnp.max(top, axis=1, keepdims=True) * factor, (BLK, width))

    def weigh(u, count, top):
        total = None
        for n in range(count):
            w = jnp.exp2(scores[u][:, n * BLK : (n + 1) * BLK] * factor - top)
            total = w if total is None else total + w
            weights[u][:, n * BLK : (n + 1) * BLK] = w.astype(jnp.bfloat16)
        return jnp.broadcast_to(jnp.sum(total, axis=1, keepdims=True), (BLK, width))

    def near_entry(i, h, n):
        offset = table_s[0, h, n]
        return REACH * blocks + i - offset, jnp.where(base + i >= offset, 0.0, NEG)

    def near_scores(k, h, u):
        i = row_block(k)
        q = query(early_q, k, h)
        own = jnp.dot(q, near[REACH * blocks + i, 0], preferred_element_type=jnp.float32)
        scores[u][:, :BLK] = jnp.where(causal, own, NEG)
        for n in range(0, listed, 2):
            (a, bias_a), (b, bias_b) = near_entry(i, h, n), near_entry(i, h, n + 1)
            sa, sb = pair_scores(q, near, a, b, bias_a, bias_b)
            scores[u][:, (n + 1) * BLK : (n + 2) * BLK] = sa
            scores[u][:, (n + 2) * BLK : (n + 3) * BLK] = sb

    def near_weigh(step, u):
        top_ref[step] = row_top(u, listed + 1)
        total_ref[step] = weigh(u, listed + 1, top_ref[step])

    def near_mix(step, u):
        i, h = row_block(step // heads), step % heads
        mixed = jnp.dot(
            weights[u][:, :BLK], near[REACH * blocks + i, 1], preferred_element_type=jnp.float32
        )
        for n in range(0, listed, 2):
            a, b = near_entry(i, h, n)[0], near_entry(i, h, n + 1)[0]
            mixed = mixed + pair_mix(u, n + 1, near, a, b)
        mixed_ref[step] = mixed

    def far_bias(own, h, block):
        gap = own - block
        ok = gap > 0
        for n in range(listed):
            ok = ok & (gap != table_s[0, h, n])
        return jnp.where(ok, 0.0, NEG)

    def far_scores(step, u):
        i, h = row_block(step // heads), step % heads
        q = query(early_q, step // heads, h)
        top = None
        for n in range(0, listed, 2):
            bias = [far_bias(base + i, h, table_s[1, h, n + d]) for d in range(2)]
            sa, sb = pair_scores(q, far, found_s[h, n], found_s[h, n + 1], *bias)
            scores[u][:, n * BLK : (n + 1) * BLK] = sa
            scores[u][:, (n + 1) * BLK : (n + 2) * BLK] = sb
            both = jnp.maximum(sa, sb)
            top = both if top is None else jnp.maximum(top, both)
        top = jnp.max(top, axis=1, keepdims=True) * factor
        tops[u] = jnp.maximum(jnp.broadcast_to(top, (BLK, width)), top_ref[step])

    def far_mix(step, u):
        i, h = row_block(step // heads), step % heads
        top = tops[u]
        scale = jnp.exp2(top_ref[step] - top)
        total, mixed = None, None
        for n in range(0, listed, 2):
            wa = jnp.exp2(scores[u][:, n * BLK : (n + 1) * BLK] * factor - top)
            wb = jnp.exp2(scores[u][:, (n + 1) * BLK : (n + 2) * BLK] * factor - top)
            total = wa + wb if total is None else total + (wa + wb)
            part = jnp.dot(
                jnp.concatenate([wa.astype(jnp.bfloat16), wb.astype(jnp.bfloat16)], axis=1),
                jnp.concatenate([far[found_s[h, n], 1], far[found_s[h, n + 1], 1]], axis=0),
                preferred_element_type=jnp.float32,
            )
            mixed = part if mixed is None else mixed + part
        total = jnp.sum(total, axis=1, keepdims=True) + total_ref[step] * scale
        mixed = mixed + mixed_ref[step] * scale
        rows = pl.ds(pl.multiple_of(i * BLK, BLK), BLK)
        staged[rows, pl.ds(pl.multiple_of(h * width, width), width)] = (mixed / total).astype(jnp.bfloat16)

    part = heads * width // 2

    def out_refs(k, c):
        i = row_block(k)
        here = staged.at[
            pl.ds(pl.multiple_of(i * BLK, BLK), BLK), pl.ds(pl.multiple_of(c * part, part), part)
        ]
        first = pl.multiple_of((group * 2 + c) * part, part)
        return here, out_ref.at[pl.ds(pl.multiple_of(k % 2 * BLK, BLK), BLK), pl.ds(first, part)]

    def out_copy(k, c):
        here, there = out_refs(k, c)
        return pltpu.make_async_remote_copy(
            here, there, out_send.at[k * 2 + c], out_recv.at[group * 4 + k % 2 * 2 + c],
            device_id=owner_of(row_block(k) // 2), device_id_type=MESH,
        )

    def out_keep(k, c):
        here, there = out_refs(k, c)
        return pltpu.make_async_copy(here, there, out_local.at[k % 2 * 2 + c])

    def kept_here(k):
        return native & (row_block(k) // 2 == head)

    def out_in(of_group, n, c):
        return pltpu.make_async_remote_copy(
            staged.at[pl.ds(0, BLK), pl.ds(0, part)],
            out_ref.at[pl.ds(n * BLK, BLK), pl.ds((of_group * 2 + c) * part, part)],
            out_send.at[0], out_recv.at[of_group * 4 + n * 2 + c],
            device_id=worker_of(jnp.int32(of_group)), device_id_type=MESH,
        )

    def send_part(k, c):
        @pl.when(kept_here(k))
        def _():
            out_keep(k, c).start()

        @pl.when(jnp.logical_not(kept_here(k)))
        def _():
            out_copy(k, c).start()

    def near_steps(k, j, carry):
        first = k * heads + 4 * j
        for u in range(4):
            near_scores(k, 4 * j + u, u)
            near_weigh(lax.rem(first + kept + u - 1, kept), (u + 3) % 4)
            near_mix(lax.rem(first + kept + u - 2, kept), (u + 2) % 4)
        return carry

    def near_group(ks):
        for k in ks:
            lax.fori_loop(0, heads // 4, functools.partial(near_steps, k), 0)
            for name in LATER[k] if k < len(LATER) else []:
                if name == "xp":

                    @pl.when(z == SIDE - 1)
                    def _():
                        event("xp")
                        send(("zpB", -1)).start()

                elif name == "zp":

                    @pl.when(z == 0)
                    def _():
                        event("zp")

                else:
                    event(name)
        last = (ks[-1] + 1) * heads
        near_weigh(jnp.int32(last - 1), 3)
        for u in (2, 3):
            near_mix(jnp.int32(last - 4 + u), u)

    def far_group(ks):
        count, before = len(ks) * heads, ks[0] * heads

        def far_steps(j, carry):
            first = 4 * j
            for u in range(4):
                far_scores(before + lax.rem(first + u + 2, count), (u + 2) % 4)
                far_mix(before + first + u, u)

            send_part(ks[0] + j // 2, j % 2)
            return carry

        for u in range(2):
            far_scores(jnp.int32(before + u), u)
        lax.fori_loop(0, count // 4, far_steps, 0)

    def full_scores(step, u):
        k, h = step // heads, step % heads
        i = row_block(k)
        q = query(late_q, k - EARLY, h)
        own = jnp.dot(q, near[REACH * blocks + i, 0], preferred_element_type=jnp.float32)
        own = jnp.where(causal, own, NEG)
        scores[u][:, :BLK] = own
        top = own
        for n in range(0, 2 * listed, 2):
            if n < listed:
                ref = near
                (a, bias_a), (b, bias_b) = near_entry(i, h, n), near_entry(i, h, n + 1)
            else:
                ref, m = far, n - listed
                a, b = found_s[h, m], found_s[h, m + 1]
                bias_a, bias_b = (far_bias(base + i, h, table_s[1, h, m + d]) for d in range(2))
            sa, sb = pair_scores(q, ref, a, b, bias_a, bias_b)
            scores[u][:, (n + 1) * BLK : (n + 2) * BLK] = sa
            scores[u][:, (n + 2) * BLK : (n + 3) * BLK] = sb
            top = jnp.maximum(top, jnp.maximum(sa, sb))
        tops[u] = jnp.broadcast_to(jnp.max(top, axis=1, keepdims=True) * factor, (BLK, width))

    def full_mix(step, u):
        i, h = row_block(step // heads), step % heads
        top = tops[u]

        def weight(n):
            return jnp.exp2(scores[u][:, n * BLK : (n + 1) * BLK] * factor - top)

        total = weight(0)
        mixed = jnp.dot(
            total.astype(jnp.bfloat16), near[REACH * blocks + i, 1], preferred_element_type=jnp.float32
        )
        for n in range(0, 2 * listed, 2):
            if n < listed:
                ref, a, b = near, near_entry(i, h, n)[0], near_entry(i, h, n + 1)[0]
            else:
                ref, a, b = far, found_s[h, n - listed], found_s[h, n - listed + 1]
            wa, wb = weight(n + 1), weight(n + 2)
            total = total + (wa + wb)
            mixed = mixed + jnp.dot(
                jnp.concatenate([wa.astype(jnp.bfloat16), wb.astype(jnp.bfloat16)], axis=1),
                jnp.concatenate([ref[a, 1], ref[b, 1]], axis=0),
                preferred_element_type=jnp.float32,
            )
        total = jnp.sum(total, axis=1, keepdims=True)
        rows = pl.ds(pl.multiple_of(i * BLK, BLK), BLK)
        staged[rows, pl.ds(pl.multiple_of(h * width, width), width)] = (mixed / total).astype(jnp.bfloat16)

    def full_group(ks):
        count, before = len(ks) * heads, ks[0] * heads

        def full_steps(j, carry):
            first = 4 * j
            for u in range(4):
                full_scores(before + lax.rem(first + u + 2, count), (u + 2) % 4)
                full_mix(before + first + u, u)
            send_part(ks[0] + j // 2, j % 2)
            return carry

        for u in range(2):
            full_scores(jnp.int32(before + u), u)
        lax.fori_loop(0, count // 4, full_steps, 0)

    for k in range(EARLY):
        wait_input(first_query + k)
    near_group(range(EARLY))
    for name in NAMES:
        share(name, 1 - core).wait_recv()
    share("own", 1 - core).wait_recv()
    far_group(range(EARLY))
    for k in range(EARLY, blocks):
        wait_input(first_query + k)
    full_group(range(EARLY, blocks))

    @pl.when(jnp.logical_not(native))
    def _():
        for k in range(len(sources)):
            swap(k).wait_send()

    for c in range(2):
        hop_one(c).wait_send()
        twin_one(c, True).wait_send()
        twin_two(c, True).wait_send()
    hop_two(1).wait_send()

    @pl.when(core == 1)
    def _():
        hop_two(0).wait_send()

    for name in NAMES:
        share(name, core).wait_send()
        if name != "zp":
            send(name).wait_send()

    @pl.when(z == SIDE - 1)
    def _():
        send("zp").wait_send()

    share("own", core).wait_send()

    for k in range(blocks):

        @pl.when(kept_here(k))
        def _():
            for c in range(2):
                out_keep(k, c).wait()

        @pl.when(jnp.logical_not(kept_here(k)))
        def _():
            for c in range(2):
                out_copy(k, c).wait_send()

    for of_group in range(4):

        @pl.when(jnp.logical_not(native & (group == of_group)))
        def _():
            for n in range(2):
                for c in range(2):
                    out_in(of_group, n, c).wait_recv()


def shards(queries, keys, values, vertical, slash):
    width = keys.shape[1]
    rows = queries.shape[0]
    blocks = rows // BLK
    heads, listed = vertical.shape
    groups = lax.axis_size("head")
    k = keys.reshape(blocks, BLK, width)
    v = values.reshape(blocks, BLK, width)
    dma = pltpu.SemaphoreType.DMA
    anywhere = pl.BlockSpec(memory_space=pl.ANY)
    bf16, f32 = jnp.bfloat16, jnp.float32
    inputs = 6 + blocks
    full_width = (2 * listed + 1) * BLK
    return pl.pallas_call(
        functools.partial(layer_kernel, blocks=blocks, heads=heads, width=width, listed=listed),
        in_specs=[anywhere] * 5,
        out_specs=anywhere,
        out_shape=jax.ShapeDtypeStruct((rows // groups, groups * heads * width), bf16),
        scratch_shapes=[
            pltpu.VMEM((2, heads, listed), jnp.int32),
            pltpu.SMEM((2, heads, listed), jnp.int32),
            pltpu.VMEM((heads, listed), jnp.int32),
            pltpu.SMEM((heads, listed), jnp.int32),
            pltpu.SMEM((2, CAP), jnp.int32),
            pltpu.VMEM((EARLY * BLK, heads * width), bf16),
            pltpu.VMEM((rows - EARLY * BLK, heads * width), bf16),
            pltpu.VMEM((blocks, BLK, width), bf16),
            pltpu.VMEM((blocks, 2, BLK, width), bf16),
            pltpu.VMEM((blocks, 2, BLK, width), bf16),
            pltpu.VMEM(((REACH + 1) * blocks, 2, BLK, width), bf16),
            pltpu.VMEM((2 * NODES * CAP, 2, BLK, width), bf16),
            pltpu.VMEM(queries.shape, bf16),
            pltpu.VMEM((heads * EARLY, BLK, width), f32),
            pltpu.VMEM((heads * EARLY, BLK, width), f32),
            pltpu.VMEM((heads * EARLY, BLK, width), f32),
            pltpu.VMEM((BLK, full_width), f32),
            pltpu.VMEM((BLK, full_width), f32),
            pltpu.VMEM((BLK, full_width), f32),
            pltpu.VMEM((BLK, full_width), f32),
            pltpu.VMEM((BLK, full_width), bf16),
            pltpu.VMEM((BLK, full_width), bf16),
            pltpu.VMEM((BLK, full_width), bf16),
            pltpu.VMEM((BLK, full_width), bf16),
            pltpu.VMEM((4, BLK, width), f32),
            dma((inputs,)),
            dma((inputs,)),
            dma((inputs,)),
            dma((2,)),
            dma((8,)),
            dma((8,)),
            dma((len(NAMES),)),
            dma((len(NAMES),)),
            dma((len(NAMES) + 1,)),
            dma((len(NAMES) + 1,)),
            dma((4,)),
            dma((2 * blocks,)),
            dma((4 * groups,)),
        ],
        compiler_params=pltpu.CompilerParams(
            collective_id=0, has_side_effects=True, vmem_limit_bytes=62 * 1024 * 1024
        ),
    )(slash, vertical, queries, k, v)


def solution(mesh):
    in_specs = (
        P("seq", "head"),
        P("seq", "head"),
        P("seq", "head"),
        P("head", None),
        P("head", None),
    )
    out_specs = P(("seq", "head"), None)
    return jax.shard_map(shards, mesh=mesh, in_specs=in_specs, out_specs=out_specs, check_vma=False)
```

```python
import functools
import math

import jax
import jax.numpy as jnp
from jax import lax
from jax.experimental import pallas as pl
from jax.experimental.pallas import tpu as pltpu
from jax.sharding import PartitionSpec as P

BLK = 128
LARGEST_OFFSET = 28
CAP = 4
NEG = -1e30
SIDE = 4
NODES = SIDE * SIDE
REACH = 4
HALF = CAP // 2
EARLY = 6
MESH = pl.DeviceIdType.MESH

COPIES = {}
COPIES["zm"] = ((0, -1), (0, 0), "full")
COPIES["xp"] = ((1, 0), (0, 0), "full")
COPIES["xm"] = ((-1, 0), (0, 0), "full")
COPIES["zm2"] = ((0, -1), (0, 1), "full")
COPIES["zp"] = ((0, 1), (0, 0), "full")
COPIES["xm2"] = ((-1, 0), (1, 0), "full")
for d in (1, -1, 2):
    COPIES["xpA", d] = ((1, 0), (0, d), "A")
    COPIES["xmA", d] = ((-1, 0), (0, d), "A")
    COPIES["xmA2", d] = ((-1, 0), (1, d), "A")
    COPIES["zpB", d] = ((0, 1), (d, 0), "B")
    COPIES["zmB", d] = ((0, -1), (d, 0), "B")
    COPIES["zmB2", d] = ((0, -1), (d, 1), "B")
NAMES = list(COPIES)

THEN = {name: [] for name in NAMES}
THEN["zm"] = ["zm2", ("xpA", 1), ("xmA", 1)]
THEN["zm2"] = [("xpA", 2), ("xmA", 2)]
THEN["zp"] = [("xpA", -1), ("xmA", -1)]
THEN["xm"] = ["xm2", ("zmB", 1)]
THEN["xp"] = [("zmB", -1), ("zpB", -1)]
THEN["xm2"] = [("zmB", 2), ("zpB", 2)]
for d in (1, -1, 2):
    THEN["xmA", d] = [("xmA2", d)]
    THEN["zmB", d] = [("zmB2", d)]

FIRST = ["zm", "xm"]
SECOND = ["zm2", "xm2", ("zmB", 1), ("xmA", 1)]
LATER = [
    ["xp", "zp", ("xmA", 2), ("zmB", 2), ("zmB2", 1), ("xmA2", 1)],
    [("zmB", -1)],
    [("xmA", -1)],
    [("zmB2", 2), ("xmA2", 2)],
    [("xmA2", -1), ("zmB2", -1)] + [(name, d) for d in (1, -1, 2) for name in ("xpA", "zpB")],
]


def layer_kernel(
    slash_ref,
    vertical_ref,
    queries_ref,
    k_ref,
    v_ref,
    out_ref,
    table_v,
    table_s,
    found_v,
    found_s,
    picked_s,
    early_q,
    late_q,
    keys_v,
    own_ref,
    hop_ref,
    near,
    far,
    staged,
    mixed_ref,
    top_ref,
    total_ref,
    scores_0,
    scores_1,
    scores_2,
    scores_3,
    weights_0,
    weights_1,
    weights_2,
    weights_3,
    tops,
    load_sem,
    swap_send,
    swap_recv,
    table_sem,
    near_send,
    near_recv,
    unit_send,
    unit_recv,
    twin_send,
    twin_recv,
    out_local,
    out_send,
    out_recv,
    *,
    blocks,
    heads,
    width,
    listed,
):
    seq, head = lax.axis_index("seq"), lax.axis_index("head")
    node, low = seq // 2, seq % 2
    high, core = head // 2, head % 2
    x, z = node // SIDE, node % SIDE
    group, slab = 2 * high + low, 2 * node + core
    native = low == core
    scores = (scores_0, scores_1, scores_2, scores_3)
    weights = (weights_0, weights_1, weights_2, weights_3)
    half = blocks // 2

    def at(dx, dz):
        to = lax.rem(x + dx + SIDE, SIDE) * SIDE + lax.rem(z + dz + SIDE, SIDE)
        return {"seq": 2 * to + low}

    follower = {"seq": 2 * lax.rem(node + 1, NODES) + low}
    leader = {"seq": 2 * lax.rem(node + NODES - 1, NODES) + low}
    twin = {"head": 2 * high + 1 - core}
    counterpart = {"seq": 2 * node + core, "head": 2 * high + low}

    def owner_of(quarter):
        return {"seq": slab, "head": quarter}

    def worker_of(of_group):
        return {"seq": 2 * node + lax.rem(of_group, 2), "head": 2 * (of_group // 2) + low}

    def row_block(k):
        near_turn = k % 2
        quarter = 2 * ((1 - near_turn) * (1 - high) + near_turn * high) + k // 4
        return 2 * quarter + k // 2 % 2

    sources = [slash_ref, vertical_ref]
    targets = [table_v.at[0], table_v.at[1]]
    for c in (1, 0):
        part = pl.ds(c * half, half)
        sources += [k_ref.at[part], v_ref.at[part]]
        targets += [keys_v.at[part], own_ref.at[part, 1]]
    first_query = len(sources)
    for k in range(blocks):
        rows = pl.ds(pl.multiple_of(row_block(k) * BLK, BLK), BLK)
        sources.append(queries_ref.at[rows])
        ref, place = (early_q, k) if k < EARLY else (late_q, k - EARLY)
        targets.append(ref.at[pl.ds(place * BLK, BLK)])

    def load(k):
        return pltpu.make_async_copy(sources[k], targets[k], load_sem.at[k])

    def swap(k):
        return pltpu.make_async_remote_copy(
            sources[k], targets[k], swap_send.at[k], swap_recv.at[k],
            device_id=counterpart, device_id_type=MESH,
        )

    def wait_input(k):
        @pl.when(native)
        def _():
            load(k).wait()

        @pl.when(jnp.logical_not(native))
        def _():
            swap(k).wait_recv()

    def prepare(wait_table):
        for k in range(2):
            wait_table(k)
        to_scalars = pltpu.make_async_copy(table_v, table_s, table_sem.at[0])
        to_scalars.start()
        to_scalars.wait()

        def note_used(h, used):
            for n in range(listed):
                block = table_s[1, h, n] - (slab - 2) * blocks
                used = tuple(
                    u | (block == (j if j < blocks else j + blocks)).astype(jnp.int32)
                    for j, u in enumerate(used)
                )
            return used

        used = lax.fori_loop(0, heads, note_used, (jnp.int32(0),) * (2 * blocks))

        def choose(used):
            picked, rank = [jnp.int32(0)] * CAP, jnp.int32(0)
            for j in range(blocks):
                picked = [
                    jnp.where((used[j] == 1) & (rank == k), j, at_k) for k, at_k in enumerate(picked)
                ]
                rank = rank + used[j]
            return picked

        for c in range(2):
            for k, block in enumerate(choose(used[c * blocks : (c + 1) * blocks])):
                picked_s[c, k] = block

        verticals = table_v[1]
        first_of = verticals // blocks * blocks
        seen = jnp.zeros_like(verticals)
        for h in range(heads):
            for n in range(listed):
                there = table_s[1, h, n] - first_of
                for j in range(blocks - 1):
                    seen = seen | jnp.where(there == j, 1 << j, 0)
        before = verticals - first_of
        place = jnp.zeros_like(verticals)
        for j in range(blocks - 1):
            place = place + jnp.where((before > j) & (seen & (1 << j) != 0), 1, 0)
        of_slab = verticals // blocks
        found_v[...] = ((of_slab % 2) * NODES + of_slab // 2) * CAP + place
        to_found = pltpu.make_async_copy(found_v, found_s, table_sem.at[1])
        to_found.start()
        to_found.wait()

    @pl.when(native)
    def _():
        for k in range(len(sources)):
            load(k).start()

    barrier = pltpu.get_barrier_semaphore()

    def greet(device):
        pl.semaphore_signal(barrier, 1, device_id=device, device_id_type=MESH)

    for device in (at(1, 0), at(-1, 0), at(0, 1), at(0, -1), follower, leader, twin):
        greet(device)
    for k in range(4):

        @pl.when(jnp.logical_not(native & (head == k)))
        def _():
            greet(owner_of(k))

        @pl.when(jnp.logical_not(native & (group == k)))
        def _():
            greet(worker_of(jnp.int32(k)))

    @pl.when(jnp.logical_not(native))
    def _():
        greet(counterpart)

    @pl.when(native)
    def _():
        prepare(lambda k: load(k).wait())

    pl.semaphore_wait(barrier, 7 + 6 + 3 * (low - core) * (low - core))

    @pl.when(jnp.logical_not(native))
    def _():
        for k in range(len(sources)):
            swap(k).start()
        prepare(lambda k: swap(k).wait_recv())

    def near_copy(src, dst, k, device):
        return pltpu.make_async_remote_copy(
            src, dst, near_send.at[k], near_recv.at[k], device_id=device, device_id_type=MESH
        )

    def near_part(back, c):
        return near.at[pl.ds((REACH - back) * blocks + c * half, half)]

    def hop_one(c):
        part = pl.ds(c * half, half)
        return near_copy(own_ref.at[part], hop_ref.at[part], c, follower)

    def hop_two(c):
        return near_copy(hop_ref.at[pl.ds(c * half, half)], near_part(4, c), 2 + c, follower)

    def twin_one(c, from_own):
        src = (own_ref if from_own else hop_ref).at[pl.ds(c * half, half)]
        return near_copy(src, near_part(1, c), 4 + c, twin)

    def twin_two(c, from_hop):
        src = hop_ref.at[pl.ds(c * half, half)] if from_hop else near_part(4, c)
        return near_copy(src, near_part(3, c), 6 + c, twin)

    def unit(dx, dz, part, of_core):
        to = lax.rem(x + dx + SIDE, SIDE) * SIDE + lax.rem(z + dz + SIDE, SIDE)
        first = (of_core * NODES + to) * CAP
        if part == "full":
            return far.at[pl.ds(pl.multiple_of(first, CAP), CAP)]
        if part == "B":
            first = first + HALF
        return far.at[pl.ds(pl.multiple_of(first, HALF), HALF)]

    def arrives(name):
        (sx, sz), (dx, dz), part = COPIES[name]
        return dx - sx, dz - sz, part

    def send(name):
        (sx, sz), (dx, dz), part = COPIES[name]
        ref, k = unit(dx, dz, part, core), NAMES.index(name)
        return pltpu.make_async_remote_copy(
            ref, ref, unit_send.at[k], unit_recv.at[k], device_id=at(sx, sz), device_id_type=MESH
        )

    def receive(name):
        (sx, sz), _, _ = COPIES[name]
        ref, k = unit(*arrives(name), core), NAMES.index(name)
        return pltpu.make_async_remote_copy(
            ref, ref, unit_send.at[k], unit_recv.at[k], device_id=at(-sx, -sz), device_id_type=MESH
        )

    def share(name, of_core):
        ref = unit(0, 0, "full", of_core) if name == "own" else unit(*arrives(name), of_core)
        k = len(NAMES) if name == "own" else NAMES.index(name)
        return pltpu.make_async_remote_copy(
            ref, ref, twin_send.at[k], twin_recv.at[k], device_id=twin, device_id_type=MESH
        )

    def start(name):
        if name[0] == "zpB":
            return
        if name == "xp" or name[0] == "xpA":

            @pl.when(z < SIDE - 1)
            def _():
                send(name).start()

        else:
            send(name).start()

    def event(name):
        receive(name).wait_recv()
        for following in THEN[name]:
            start(following)
        share(name, core).start()

    def pack(src, node_of, c):
        first = pl.multiple_of((core * NODES + node_of) * CAP, CAP)
        for k in range(CAP):
            for kv in range(2):
                far[first + k, kv] = src[picked_s[c, k], kv]

    for c in (1, 0):
        for k in range(2):
            wait_input(2 + 2 * (1 - c) + k)
        for j in range(c * half, (c + 1) * half):
            own_ref[j, 0] = keys_v[j].T
        hop_one(c).start()

        @pl.when(core == 0)
        def _():
            twin_one(c, True).start()

    pack(own_ref, node, 1)
    for j in range(blocks):
        for kv in range(2):
            near[REACH * blocks + j, kv] = own_ref[j, kv]
    for name in ("zm", "xm", "xp"):
        start(name)
    share("own", core).start()

    for name in FIRST:
        event(name)
    for c in (1, 0):
        hop_one(c).wait_recv()
        if c == 1:
            hop_two(c).start()
        else:

            @pl.when(core == 1)
            def _():
                hop_two(c).start()

        @pl.when(core == 1)
        def _():
            twin_one(c, False).start()

        @pl.when(core == 0)
        def _():
            twin_two(c, True).start()

    @pl.when(z > 0)
    def _():
        pack(hop_ref, x * SIDE + z - 1, 0)

    for j in range(blocks):
        for kv in range(2):
            near[2 * blocks + j, kv] = hop_ref[j, kv]

    @pl.when(z > 0)
    def _():
        for following in THEN["zp"]:
            start(following)
        share("zp", core).start()

    @pl.when(z == SIDE - 1)
    def _():
        send("zp").start()
        send("xp").start()

    @pl.when(z < SIDE - 1)
    def _():
        event("xp")

    for name in SECOND:
        event(name)

    @pl.when(core == 1)
    def _():
        for c in (1, 0):
            hop_two(c).wait_recv()
            twin_two(c, False).start()

    @pl.when(core == 0)
    def _():
        hop_two(1).wait_recv()

    for c in range(2):
        twin_one(c, True).wait_recv()
        twin_two(c, True).wait_recv()

    for d in (1, 2):
        send(("zpB", d)).start()

    @pl.when(z < SIDE - 1)
    def _():
        send(("zpB", -1)).start()

    @pl.when(z == SIDE - 1)
    def _():
        for d in (1, -1, 2):
            send(("xpA", d)).start()

    factor = math.log2(math.e) / math.sqrt(width)
    causal = lax.broadcasted_iota(jnp.int32, (BLK, BLK), 0) >= lax.broadcasted_iota(
        jnp.int32, (BLK, BLK), 1
    )
    kept = heads * EARLY
    base = slab * blocks

    def query(ref, k, h):
        return ref[
            pl.ds(pl.multiple_of(k * BLK, BLK), BLK),
            pl.ds(pl.multiple_of(h * width, width), width),
        ]

    def pair_scores(q, ref, a, b, bias_a, bias_b):
        pair = jnp.dot(
            q, jnp.concatenate([ref[a, 0], ref[b, 0]], axis=1), preferred_element_type=jnp.float32
        )
        return pair[:, :BLK] + bias_a, pair[:, BLK:] + bias_b

    def pair_mix(u, n, ref, a, b):
        return jnp.dot(
            weights[u][:, n * BLK : (n + 2) * BLK],
            jnp.concatenate([ref[a, 1], ref[b, 1]], axis=0),
            preferred_element_type=jnp.float32,
        )

    def row_top(u, count):
        top = scores[u][:, :BLK]
        for n in range(1, count):
            top = jnp.maximum(top, scores[u][:, n * BLK : (n + 1) * BLK])
        return jnp.broadcast_to(jnp.max(top, axis=1, keepdims=True) * factor, (BLK, width))

    def weigh(u, count, top):
        total = None
        for n in range(count):
            w = jnp.exp2(scores[u][:, n * BLK : (n + 1) * BLK] * factor - top)
            total = w if total is None else total + w
            weights[u][:, n * BLK : (n + 1) * BLK] = w.astype(jnp.bfloat16)
        return jnp.broadcast_to(jnp.sum(total, axis=1, keepdims=True), (BLK, width))

    def near_entry(i, h, n):
        offset = table_s[0, h, n]
        return REACH * blocks + i - offset, jnp.where(base + i >= offset, 0.0, NEG)

    def near_scores(k, h, u):
        i = row_block(k)
        q = query(early_q, k, h)
        own = jnp.dot(q, near[REACH * blocks + i, 0], preferred_element_type=jnp.float32)
        scores[u][:, :BLK] = jnp.where(causal, own, NEG)
        for n in range(0, listed, 2):
            (a, bias_a), (b, bias_b) = near_entry(i, h, n), near_entry(i, h, n + 1)
            sa, sb = pair_scores(q, near, a, b, bias_a, bias_b)
            scores[u][:, (n + 1) * BLK : (n + 2) * BLK] = sa
            scores[u][:, (n + 2) * BLK : (n + 3) * BLK] = sb

    def near_weigh(step, u):
        top_ref[step] = row_top(u, listed + 1)
        total_ref[step] = weigh(u, listed + 1, top_ref[step])

    def near_mix(step, u):
        i, h = row_block(step // heads), step % heads
        mixed = jnp.dot(
            weights[u][:, :BLK], near[REACH * blocks + i, 1], preferred_element_type=jnp.float32
        )
        for n in range(0, listed, 2):
            a, b = near_entry(i, h, n)[0], near_entry(i, h, n + 1)[0]
            mixed = mixed + pair_mix(u, n + 1, near, a, b)
        mixed_ref[step] = mixed

    def far_bias(own, h, block):
        gap = own - block
        ok = gap > 0
        for n in range(listed):
            ok = ok & (gap != table_s[0, h, n])
        return jnp.where(ok, 0.0, NEG)

    def far_scores(step, u):
        i, h = row_block(step // heads), step % heads
        q = query(early_q, step // heads, h)
        top = None
        for n in range(0, listed, 2):
            bias = [far_bias(base + i, h, table_s[1, h, n + d]) for d in range(2)]
            sa, sb = pair_scores(q, far, found_s[h, n], found_s[h, n + 1], *bias)
            scores[u][:, n * BLK : (n + 1) * BLK] = sa
            scores[u][:, (n + 1) * BLK : (n + 2) * BLK] = sb
            both = jnp.maximum(sa, sb)
            top = both if top is None else jnp.maximum(top, both)
        top = jnp.max(top, axis=1, keepdims=True) * factor
        tops[u] = jnp.maximum(jnp.broadcast_to(top, (BLK, width)), top_ref[step])

    def far_mix(step, u):
        i, h = row_block(step // heads), step % heads
        top = tops[u]
        scale = jnp.exp2(top_ref[step] - top)
        total, mixed = None, None
        for n in range(0, listed, 2):
            wa = jnp.exp2(scores[u][:, n * BLK : (n + 1) * BLK] * factor - top)
            wb = jnp.exp2(scores[u][:, (n + 1) * BLK : (n + 2) * BLK] * factor - top)
            total = wa + wb if total is None else total + (wa + wb)
            part = jnp.dot(
                jnp.concatenate([wa.astype(jnp.bfloat16), wb.astype(jnp.bfloat16)], axis=1),
                jnp.concatenate([far[found_s[h, n], 1], far[found_s[h, n + 1], 1]], axis=0),
                preferred_element_type=jnp.float32,
            )
            mixed = part if mixed is None else mixed + part
        total = jnp.sum(total, axis=1, keepdims=True) + total_ref[step] * scale
        mixed = mixed + mixed_ref[step] * scale
        rows = pl.ds(pl.multiple_of(i * BLK, BLK), BLK)
        staged[rows, pl.ds(pl.multiple_of(h * width, width), width)] = (mixed / total).astype(jnp.bfloat16)

    part = heads * width // 2

    def out_refs(k, c):
        i = row_block(k)
        here = staged.at[
            pl.ds(pl.multiple_of(i * BLK, BLK), BLK), pl.ds(pl.multiple_of(c * part, part), part)
        ]
        first = pl.multiple_of((group * 2 + c) * part, part)
        return here, out_ref.at[pl.ds(pl.multiple_of(k // 2 % 2 * BLK, BLK), BLK), pl.ds(first, part)]

    def out_copy(k, c):
        here, there = out_refs(k, c)
        return pltpu.make_async_remote_copy(
            here, there, out_send.at[k * 2 + c], out_recv.at[group * 4 + k // 2 % 2 * 2 + c],
            device_id=owner_of(row_block(k) // 2), device_id_type=MESH,
        )

    def out_keep(k, c):
        here, there = out_refs(k, c)
        return pltpu.make_async_copy(here, there, out_local.at[k // 2 % 2 * 2 + c])

    def kept_here(k):
        return native & (row_block(k) // 2 == head)

    def out_in(of_group, n, c):
        return pltpu.make_async_remote_copy(
            staged.at[pl.ds(0, BLK), pl.ds(0, part)],
            out_ref.at[pl.ds(n * BLK, BLK), pl.ds((of_group * 2 + c) * part, part)],
            out_send.at[0], out_recv.at[of_group * 4 + n * 2 + c],
            device_id=worker_of(jnp.int32(of_group)), device_id_type=MESH,
        )

    def send_part(k, c):
        @pl.when(kept_here(k))
        def _():
            out_keep(k, c).start()

        @pl.when(jnp.logical_not(kept_here(k)))
        def _():
            out_copy(k, c).start()

    def near_steps(k, j, carry):
        first = k * heads + 4 * j
        for u in range(4):
            near_scores(k, 4 * j + u, u)
            near_weigh(lax.rem(first + kept + u - 1, kept), (u + 3) % 4)
            near_mix(lax.rem(first + kept + u - 2, kept), (u + 2) % 4)
        return carry

    def near_group(ks):
        for k in ks:
            lax.fori_loop(0, heads // 4, functools.partial(near_steps, k), 0)
            for name in LATER[k] if k < len(LATER) else []:
                if name == "xp":

                    @pl.when(z == SIDE - 1)
                    def _():
                        event("xp")
                        send(("zpB", -1)).start()

                elif name == "zp":

                    @pl.when(z == 0)
                    def _():
                        event("zp")

                else:
                    event(name)
        last = (ks[-1] + 1) * heads
        near_weigh(jnp.int32(last - 1), 3)
        for u in (2, 3):
            near_mix(jnp.int32(last - 4 + u), u)

    def far_group(ks):
        count, before = len(ks) * heads, ks[0] * heads

        def far_steps(j, carry):
            first = 4 * j
            for u in range(4):
                far_scores(before + lax.rem(first + u + 2, count), (u + 2) % 4)
                far_mix(before + first + u, u)

            send_part(ks[0] + j // 2, j % 2)
            return carry

        for u in range(2):
            far_scores(jnp.int32(before + u), u)
        lax.fori_loop(0, count // 4, far_steps, 0)

    def full_scores(step, u):
        k, h = step // heads, step % heads
        i = row_block(k)
        q = query(late_q, k - EARLY, h)
        own = jnp.dot(q, near[REACH * blocks + i, 0], preferred_element_type=jnp.float32)
        own = jnp.where(causal, own, NEG)
        scores[u][:, :BLK] = own
        top = own
        for n in range(0, 2 * listed, 2):
            if n < listed:
                ref = near
                (a, bias_a), (b, bias_b) = near_entry(i, h, n), near_entry(i, h, n + 1)
            else:
                ref, m = far, n - listed
                a, b = found_s[h, m], found_s[h, m + 1]
                bias_a, bias_b = (far_bias(base + i, h, table_s[1, h, m + d]) for d in range(2))
            sa, sb = pair_scores(q, ref, a, b, bias_a, bias_b)
            scores[u][:, (n + 1) * BLK : (n + 2) * BLK] = sa
            scores[u][:, (n + 2) * BLK : (n + 3) * BLK] = sb
            top = jnp.maximum(top, jnp.maximum(sa, sb))
        tops[u] = jnp.broadcast_to(jnp.max(top, axis=1, keepdims=True) * factor, (BLK, width))

    def full_mix(step, u):
        i, h = row_block(step // heads), step % heads
        top = tops[u]

        def weight(n):
            return jnp.exp2(scores[u][:, n * BLK : (n + 1) * BLK] * factor - top)

        total = weight(0)
        mixed = jnp.dot(
            total.astype(jnp.bfloat16), near[REACH * blocks + i, 1], preferred_element_type=jnp.float32
        )
        for n in range(0, 2 * listed, 2):
            if n < listed:
                ref, a, b = near, near_entry(i, h, n)[0], near_entry(i, h, n + 1)[0]
            else:
                ref, a, b = far, found_s[h, n - listed], found_s[h, n - listed + 1]
            wa, wb = weight(n + 1), weight(n + 2)
            total = total + (wa + wb)
            mixed = mixed + jnp.dot(
                jnp.concatenate([wa.astype(jnp.bfloat16), wb.astype(jnp.bfloat16)], axis=1),
                jnp.concatenate([ref[a, 1], ref[b, 1]], axis=0),
                preferred_element_type=jnp.float32,
            )
        total = jnp.sum(total, axis=1, keepdims=True)
        rows = pl.ds(pl.multiple_of(i * BLK, BLK), BLK)
        staged[rows, pl.ds(pl.multiple_of(h * width, width), width)] = (mixed / total).astype(jnp.bfloat16)

    def full_group(ks):
        count, before = len(ks) * heads, ks[0] * heads

        def full_steps(j, carry):
            first = 4 * j
            for u in range(4):
                full_scores(before + lax.rem(first + u + 2, count), (u + 2) % 4)
                full_mix(before + first + u, u)
            send_part(ks[0] + j // 2, j % 2)
            return carry

        for u in range(2):
            full_scores(jnp.int32(before + u), u)
        lax.fori_loop(0, count // 4, full_steps, 0)

    for k in range(EARLY):
        wait_input(first_query + k)
    near_group(range(EARLY))
    for name in NAMES:
        share(name, 1 - core).wait_recv()
    share("own", 1 - core).wait_recv()
    far_group(range(EARLY))
    for k in range(EARLY, blocks):
        wait_input(first_query + k)
    full_group(range(EARLY, blocks))

    @pl.when(jnp.logical_not(native))
    def _():
        for k in range(len(sources)):
            swap(k).wait_send()

    for c in range(2):
        hop_one(c).wait_send()
        twin_one(c, True).wait_send()
        twin_two(c, True).wait_send()
    hop_two(1).wait_send()

    @pl.when(core == 1)
    def _():
        hop_two(0).wait_send()

    for name in NAMES:
        share(name, core).wait_send()
        if name != "zp":
            send(name).wait_send()

    @pl.when(z == SIDE - 1)
    def _():
        send("zp").wait_send()

    share("own", core).wait_send()

    for k in range(blocks):

        @pl.when(kept_here(k))
        def _():
            for c in range(2):
                out_keep(k, c).wait()

        @pl.when(jnp.logical_not(kept_here(k)))
        def _():
            for c in range(2):
                out_copy(k, c).wait_send()

    for of_group in range(4):

        @pl.when(jnp.logical_not(native & (group == of_group)))
        def _():
            for n in range(2):
                for c in range(2):
                    out_in(of_group, n, c).wait_recv()


def shards(queries, keys, values, vertical, slash):
    width = keys.shape[1]
    rows = queries.shape[0]
    blocks = rows // BLK
    heads, listed = vertical.shape
    groups = lax.axis_size("head")
    k = keys.reshape(blocks, BLK, width)
    v = values.reshape(blocks, BLK, width)
    dma = pltpu.SemaphoreType.DMA
    anywhere = pl.BlockSpec(memory_space=pl.ANY)
    bf16, f32 = jnp.bfloat16, jnp.float32
    inputs = 6 + blocks
    full_width = (2 * listed + 1) * BLK
    return pl.pallas_call(
        functools.partial(layer_kernel, blocks=blocks, heads=heads, width=width, listed=listed),
        in_specs=[anywhere] * 5,
        out_specs=anywhere,
        out_shape=jax.ShapeDtypeStruct((rows // groups, groups * heads * width), bf16),
        scratch_shapes=[
            pltpu.VMEM((2, heads, listed), jnp.int32),
            pltpu.SMEM((2, heads, listed), jnp.int32),
            pltpu.VMEM((heads, listed), jnp.int32),
            pltpu.SMEM((heads, listed), jnp.int32),
            pltpu.SMEM((2, CAP), jnp.int32),
            pltpu.VMEM((EARLY * BLK, heads * width), bf16),
            pltpu.VMEM((rows - EARLY * BLK, heads * width), bf16),
            pltpu.VMEM((blocks, BLK, width), bf16),
            pltpu.VMEM((blocks, 2, BLK, width), bf16),
            pltpu.VMEM((blocks, 2, BLK, width), bf16),
            pltpu.VMEM(((REACH + 1) * blocks, 2, BLK, width), bf16),
            pltpu.VMEM((2 * NODES * CAP, 2, BLK, width), bf16),
            pltpu.VMEM(queries.shape, bf16),
            pltpu.VMEM((heads * EARLY, BLK, width), f32),
            pltpu.VMEM((heads * EARLY, BLK, width), f32),
            pltpu.VMEM((heads * EARLY, BLK, width), f32),
            pltpu.VMEM((BLK, full_width), f32),
            pltpu.VMEM((BLK, full_width), f32),
            pltpu.VMEM((BLK, full_width), f32),
            pltpu.VMEM((BLK, full_width), f32),
            pltpu.VMEM((BLK, full_width), bf16),
            pltpu.VMEM((BLK, full_width), bf16),
            pltpu.VMEM((BLK, full_width), bf16),
            pltpu.VMEM((BLK, full_width), bf16),
            pltpu.VMEM((4, BLK, width), f32),
            dma((inputs,)),
            dma((inputs,)),
            dma((inputs,)),
            dma((2,)),
            dma((8,)),
            dma((8,)),
            dma((len(NAMES),)),
            dma((len(NAMES),)),
            dma((len(NAMES) + 1,)),
            dma((len(NAMES) + 1,)),
            dma((4,)),
            dma((2 * blocks,)),
            dma((4 * groups,)),
        ],
        compiler_params=pltpu.CompilerParams(
            collective_id=0, has_side_effects=True, vmem_limit_bytes=62 * 1024 * 1024
        ),
    )(slash, vertical, queries, k, v)


def solution(mesh):
    in_specs = (
        P("seq", "head"),
        P("seq", "head"),
        P("seq", "head"),
        P("head", None),
        P("head", None),
    )
    out_specs = P(("seq", "head"), None)
    return jax.shard_map(shards, mesh=mesh, in_specs=in_specs, out_specs=out_specs, check_vma=False)
```

```python
import functools
import math

import jax
import jax.numpy as jnp
from jax import lax
from jax.experimental import pallas as pl
from jax.experimental.pallas import tpu as pltpu
from jax.sharding import PartitionSpec as P

BLK = 128
LARGEST_OFFSET = 28
CAP = 4
NEG = -1e30
SIDE = 4
NODES = SIDE * SIDE
REACH = 4
HALF = CAP // 2
EARLY = 5
MESH = pl.DeviceIdType.MESH

COPIES = {}
COPIES["zm"] = ((0, -1), (0, 0), "full")
COPIES["xp"] = ((1, 0), (0, 0), "full")
COPIES["xm"] = ((-1, 0), (0, 0), "full")
COPIES["zm2"] = ((0, -1), (0, 1), "full")
COPIES["zp"] = ((0, 1), (0, 0), "full")
COPIES["xm2"] = ((-1, 0), (1, 0), "full")
for d in (1, -1, 2):
    COPIES["xpA", d] = ((1, 0), (0, d), "A")
    COPIES["xmA", d] = ((-1, 0), (0, d), "A")
    COPIES["xmA2", d] = ((-1, 0), (1, d), "A")
    COPIES["zpB", d] = ((0, 1), (d, 0), "B")
    COPIES["zmB", d] = ((0, -1), (d, 0), "B")
    COPIES["zmB2", d] = ((0, -1), (d, 1), "B")
NAMES = list(COPIES)

THEN = {name: [] for name in NAMES}
THEN["zm"] = ["zm2", ("xpA", 1), ("xmA", 1)]
THEN["zm2"] = [("xpA", 2), ("xmA", 2)]
THEN["zp"] = [("xpA", -1), ("xmA", -1)]
THEN["xm"] = ["xm2", ("zmB", 1)]
THEN["xp"] = [("zmB", -1), ("zpB", -1)]
THEN["xm2"] = [("zmB", 2), ("zpB", 2)]
for d in (1, -1, 2):
    THEN["xmA", d] = [("xmA2", d)]
    THEN["zmB", d] = [("zmB2", d)]

FIRST = ["zm", "xm"]
SECOND = ["zm2", "xm2", ("zmB", 1), ("xmA", 1)]
LATER = [
    ["xp", "zp", ("xmA", 2), ("zmB", 2), ("zmB2", 1), ("xmA2", 1)],
    [("zmB", -1)],
    [("xmA", -1)],
    [("zmB2", 2), ("xmA2", 2)],
    [("xmA2", -1), ("zmB2", -1)] + [(name, d) for d in (1, -1, 2) for name in ("xpA", "zpB")],
]


def layer_kernel(
    slash_ref,
    vertical_ref,
    queries_ref,
    k_ref,
    v_ref,
    out_ref,
    table_v,
    table_s,
    found_v,
    found_s,
    picked_s,
    early_q,
    late_q,
    keys_v,
    own_ref,
    hop_ref,
    near,
    far,
    staged,
    mixed_ref,
    top_ref,
    total_ref,
    scores_0,
    scores_1,
    scores_2,
    scores_3,
    weights_0,
    weights_1,
    weights_2,
    weights_3,
    tops,
    load_sem,
    swap_send,
    swap_recv,
    table_sem,
    near_send,
    near_recv,
    unit_send,
    unit_recv,
    twin_send,
    twin_recv,
    out_local,
    out_send,
    out_recv,
    *,
    blocks,
    heads,
    width,
    listed,
):
    seq, head = lax.axis_index("seq"), lax.axis_index("head")
    node, low = seq // 2, seq % 2
    high, core = head // 2, head % 2
    x, z = node // SIDE, node % SIDE
    group, slab = 2 * high + low, 2 * node + core
    native = low == core
    scores = (scores_0, scores_1, scores_2, scores_3)
    weights = (weights_0, weights_1, weights_2, weights_3)
    half = blocks // 2

    def at(dx, dz):
        to = lax.rem(x + dx + SIDE, SIDE) * SIDE + lax.rem(z + dz + SIDE, SIDE)
        return {"seq": 2 * to + low}

    follower = {"seq": 2 * lax.rem(node + 1, NODES) + low}
    leader = {"seq": 2 * lax.rem(node + NODES - 1, NODES) + low}
    twin = {"head": 2 * high + 1 - core}
    counterpart = {"seq": 2 * node + core, "head": 2 * high + low}

    def owner_of(quarter):
        return {"seq": slab, "head": quarter}

    def worker_of(of_group):
        return {"seq": 2 * node + lax.rem(of_group, 2), "head": 2 * (of_group // 2) + low}

    def row_block(k):
        near_turn = k % 2
        quarter = 2 * ((1 - near_turn) * (1 - high) + near_turn * high) + k // 4
        return 2 * quarter + k // 2 % 2

    sources = [slash_ref, vertical_ref]
    targets = [table_v.at[0], table_v.at[1]]
    for c in (1, 0):
        part = pl.ds(c * half, half)
        sources += [k_ref.at[part], v_ref.at[part]]
        targets += [keys_v.at[part], own_ref.at[part, 1]]
    first_query = len(sources)
    for k in range(blocks):
        rows = pl.ds(pl.multiple_of(row_block(k) * BLK, BLK), BLK)
        sources.append(queries_ref.at[rows])
        ref, place = (early_q, k) if k < EARLY else (late_q, k - EARLY)
        targets.append(ref.at[pl.ds(place * BLK, BLK)])

    def load(k):
        return pltpu.make_async_copy(sources[k], targets[k], load_sem.at[k])

    def swap(k):
        return pltpu.make_async_remote_copy(
            sources[k], targets[k], swap_send.at[k], swap_recv.at[k],
            device_id=counterpart, device_id_type=MESH,
        )

    def wait_input(k):
        @pl.when(native)
        def _():
            load(k).wait()

        @pl.when(jnp.logical_not(native))
        def _():
            swap(k).wait_recv()

    def prepare(wait_table):
        for k in range(2):
            wait_table(k)
        to_scalars = pltpu.make_async_copy(table_v, table_s, table_sem.at[0])
        to_scalars.start()
        to_scalars.wait()

        def note_used(h, used):
            for n in range(listed):
                block = table_s[1, h, n] - (slab - 2) * blocks
                used = tuple(
                    u | (block == (j if j < blocks else j + blocks)).astype(jnp.int32)
                    for j, u in enumerate(used)
                )
            return used

        used = lax.fori_loop(0, heads, note_used, (jnp.int32(0),) * (2 * blocks))

        def choose(used):
            picked, rank = [jnp.int32(0)] * CAP, jnp.int32(0)
            for j in range(blocks):
                picked = [
                    jnp.where((used[j] == 1) & (rank == k), j, at_k) for k, at_k in enumerate(picked)
                ]
                rank = rank + used[j]
            return picked

        for c in range(2):
            for k, block in enumerate(choose(used[c * blocks : (c + 1) * blocks])):
                picked_s[c, k] = block

        verticals = table_v[1]
        first_of = verticals // blocks * blocks
        seen = jnp.zeros_like(verticals)
        for h in range(heads):
            for n in range(listed):
                there = table_s[1, h, n] - first_of
                for j in range(blocks - 1):
                    seen = seen | jnp.where(there == j, 1 << j, 0)
        before = verticals - first_of
        place = jnp.zeros_like(verticals)
        for j in range(blocks - 1):
            place = place + jnp.where((before > j) & (seen & (1 << j) != 0), 1, 0)
        of_slab = verticals // blocks
        found_v[...] = ((of_slab % 2) * NODES + of_slab // 2) * CAP + place
        to_found = pltpu.make_async_copy(found_v, found_s, table_sem.at[1])
        to_found.start()
        to_found.wait()

    @pl.when(native)
    def _():
        for k in range(len(sources)):
            load(k).start()

    barrier = pltpu.get_barrier_semaphore()

    def greet(device):
        pl.semaphore_signal(barrier, 1, device_id=device, device_id_type=MESH)

    for device in (at(1, 0), at(-1, 0), at(0, 1), at(0, -1), follower, leader, twin):
        greet(device)
    for k in range(4):

        @pl.when(jnp.logical_not(native & (head == k)))
        def _():
            greet(owner_of(k))

        @pl.when(jnp.logical_not(native & (group == k)))
        def _():
            greet(worker_of(jnp.int32(k)))

    @pl.when(jnp.logical_not(native))
    def _():
        greet(counterpart)

    @pl.when(native)
    def _():
        prepare(lambda k: load(k).wait())

    pl.semaphore_wait(barrier, 7 + 6 + 3 * (low - core) * (low - core))

    @pl.when(jnp.logical_not(native))
    def _():
        for k in range(len(sources)):
            swap(k).start()
        prepare(lambda k: swap(k).wait_recv())

    def near_copy(src, dst, k, device):
        return pltpu.make_async_remote_copy(
            src, dst, near_send.at[k], near_recv.at[k], device_id=device, device_id_type=MESH
        )

    def near_part(back, c):
        return near.at[pl.ds((REACH - back) * blocks + c * half, half)]

    def hop_one(c):
        part = pl.ds(c * half, half)
        return near_copy(own_ref.at[part], hop_ref.at[part], c, follower)

    def hop_two(c):
        return near_copy(hop_ref.at[pl.ds(c * half, half)], near_part(4, c), 2 + c, follower)

    def twin_one(c, from_own):
        src = (own_ref if from_own else hop_ref).at[pl.ds(c * half, half)]
        return near_copy(src, near_part(1, c), 4 + c, twin)

    def twin_two(c, from_hop):
        src = hop_ref.at[pl.ds(c * half, half)] if from_hop else near_part(4, c)
        return near_copy(src, near_part(3, c), 6 + c, twin)

    def unit(dx, dz, part, of_core):
        to = lax.rem(x + dx + SIDE, SIDE) * SIDE + lax.rem(z + dz + SIDE, SIDE)
        first = (of_core * NODES + to) * CAP
        if part == "full":
            return far.at[pl.ds(pl.multiple_of(first, CAP), CAP)]
        if part == "B":
            first = first + HALF
        return far.at[pl.ds(pl.multiple_of(first, HALF), HALF)]

    def arrives(name):
        (sx, sz), (dx, dz), part = COPIES[name]
        return dx - sx, dz - sz, part

    def send(name):
        (sx, sz), (dx, dz), part = COPIES[name]
        ref, k = unit(dx, dz, part, core), NAMES.index(name)
        return pltpu.make_async_remote_copy(
            ref, ref, unit_send.at[k], unit_recv.at[k], device_id=at(sx, sz), device_id_type=MESH
        )

    def receive(name):
        (sx, sz), _, _ = COPIES[name]
        ref, k = unit(*arrives(name), core), NAMES.index(name)
        return pltpu.make_async_remote_copy(
            ref, ref, unit_send.at[k], unit_recv.at[k], device_id=at(-sx, -sz), device_id_type=MESH
        )

    def share(name, of_core):
        ref = unit(0, 0, "full", of_core) if name == "own" else unit(*arrives(name), of_core)
        k = len(NAMES) if name == "own" else NAMES.index(name)
        return pltpu.make_async_remote_copy(
            ref, ref, twin_send.at[k], twin_recv.at[k], device_id=twin, device_id_type=MESH
        )

    def start(name):
        if name[0] == "zpB":
            return
        if name == "xp" or name[0] == "xpA":

            @pl.when(z < SIDE - 1)
            def _():
                send(name).start()

        else:
            send(name).start()

    def event(name):
        receive(name).wait_recv()
        for following in THEN[name]:
            start(following)
        share(name, core).start()

    def pack(src, node_of, c):
        first = pl.multiple_of((core * NODES + node_of) * CAP, CAP)
        for k in range(CAP):
            for kv in range(2):
                far[first + k, kv] = src[picked_s[c, k], kv]

    for c in (1, 0):
        for k in range(2):
            wait_input(2 + 2 * (1 - c) + k)
        for j in range(c * half, (c + 1) * half):
            own_ref[j, 0] = keys_v[j].T
        hop_one(c).start()

        @pl.when(core == 0)
        def _():
            twin_one(c, True).start()

    pack(own_ref, node, 1)
    for j in range(blocks):
        for kv in range(2):
            near[REACH * blocks + j, kv] = own_ref[j, kv]
    for name in ("zm", "xm", "xp"):
        start(name)
    share("own", core).start()

    for name in FIRST:
        event(name)
    for c in (1, 0):
        hop_one(c).wait_recv()
        if c == 1:
            hop_two(c).start()
        else:

            @pl.when(core == 1)
            def _():
                hop_two(c).start()

        @pl.when(core == 1)
        def _():
            twin_one(c, False).start()

        @pl.when(core == 0)
        def _():
            twin_two(c, True).start()

    @pl.when(z > 0)
    def _():
        pack(hop_ref, x * SIDE + z - 1, 0)

    for j in range(blocks):
        for kv in range(2):
            near[2 * blocks + j, kv] = hop_ref[j, kv]

    @pl.when(z > 0)
    def _():
        for following in THEN["zp"]:
            start(following)
        share("zp", core).start()

    @pl.when(z == SIDE - 1)
    def _():
        send("zp").start()
        send("xp").start()

    @pl.when(z < SIDE - 1)
    def _():
        event("xp")

    for name in SECOND:
        event(name)

    @pl.when(core == 1)
    def _():
        for c in (1, 0):
            hop_two(c).wait_recv()
            twin_two(c, False).start()

    @pl.when(core == 0)
    def _():
        hop_two(1).wait_recv()

    for c in range(2):
        twin_one(c, True).wait_recv()
        twin_two(c, True).wait_recv()

    for d in (1, 2):
        send(("zpB", d)).start()

    @pl.when(z < SIDE - 1)
    def _():
        send(("zpB", -1)).start()

    @pl.when(z == SIDE - 1)
    def _():
        for d in (1, -1, 2):
            send(("xpA", d)).start()

    factor = math.log2(math.e) / math.sqrt(width)
    causal = lax.broadcasted_iota(jnp.int32, (BLK, BLK), 0) >= lax.broadcasted_iota(
        jnp.int32, (BLK, BLK), 1
    )
    kept = heads * EARLY
    base = slab * blocks

    def query(ref, k, h):
        return ref[
            pl.ds(pl.multiple_of(k * BLK, BLK), BLK),
            pl.ds(pl.multiple_of(h * width, width), width),
        ]

    def pair_scores(q, ref, a, b, bias_a, bias_b):
        pair = jnp.dot(
            q, jnp.concatenate([ref[a, 0], ref[b, 0]], axis=1), preferred_element_type=jnp.float32
        )
        return pair[:, :BLK] + bias_a, pair[:, BLK:] + bias_b

    def pair_mix(u, n, ref, a, b):
        return jnp.dot(
            weights[u][:, n * BLK : (n + 2) * BLK],
            jnp.concatenate([ref[a, 1], ref[b, 1]], axis=0),
            preferred_element_type=jnp.float32,
        )

    def row_top(u, count):
        top = scores[u][:, :BLK]
        for n in range(1, count):
            top = jnp.maximum(top, scores[u][:, n * BLK : (n + 1) * BLK])
        return jnp.broadcast_to(jnp.max(top, axis=1, keepdims=True) * factor, (BLK, width))

    def weigh(u, count, top):
        total = None
        for n in range(count):
            w = jnp.exp2(scores[u][:, n * BLK : (n + 1) * BLK] * factor - top)
            total = w if total is None else total + w
            weights[u][:, n * BLK : (n + 1) * BLK] = w.astype(jnp.bfloat16)
        return jnp.broadcast_to(jnp.sum(total, axis=1, keepdims=True), (BLK, width))

    def near_entry(i, h, n):
        offset = table_s[0, h, n]
        return REACH * blocks + i - offset, jnp.where(base + i >= offset, 0.0, NEG)

    def near_scores(k, h, u):
        i = row_block(k)
        q = query(early_q, k, h)
        own = jnp.dot(q, near[REACH * blocks + i, 0], preferred_element_type=jnp.float32)
        scores[u][:, :BLK] = jnp.where(causal, own, NEG)
        for n in range(0, listed, 2):
            (a, bias_a), (b, bias_b) = near_entry(i, h, n), near_entry(i, h, n + 1)
            sa, sb = pair_scores(q, near, a, b, bias_a, bias_b)
            scores[u][:, (n + 1) * BLK : (n + 2) * BLK] = sa
            scores[u][:, (n + 2) * BLK : (n + 3) * BLK] = sb

    def near_weigh(step, u):
        top_ref[step] = row_top(u, listed + 1)
        total_ref[step] = weigh(u, listed + 1, top_ref[step])

    def near_mix(step, u):
        i, h = row_block(step // heads), step % heads
        mixed = jnp.dot(
            weights[u][:, :BLK], near[REACH * blocks + i, 1], preferred_element_type=jnp.float32
        )
        for n in range(0, listed, 2):
            a, b = near_entry(i, h, n)[0], near_entry(i, h, n + 1)[0]
            mixed = mixed + pair_mix(u, n + 1, near, a, b)
        mixed_ref[step] = mixed

    def far_bias(own, h, block):
        gap = own - block
        ok = gap > 0
        for n in range(listed):
            ok = ok & (gap != table_s[0, h, n])
        return jnp.where(ok, 0.0, NEG)

    def far_scores(step, u):
        i, h = row_block(step // heads), step % heads
        q = query(early_q, step // heads, h)
        top = None
        for n in range(0, listed, 2):
            bias = [far_bias(base + i, h, table_s[1, h, n + d]) for d in range(2)]
            sa, sb = pair_scores(q, far, found_s[h, n], found_s[h, n + 1], *bias)
            scores[u][:, n * BLK : (n + 1) * BLK] = sa
            scores[u][:, (n + 1) * BLK : (n + 2) * BLK] = sb
            both = jnp.maximum(sa, sb)
            top = both if top is None else jnp.maximum(top, both)
        top = jnp.max(top, axis=1, keepdims=True) * factor
        tops[u] = jnp.maximum(jnp.broadcast_to(top, (BLK, width)), top_ref[step])

    def far_mix(step, u):
        i, h = row_block(step // heads), step % heads
        top = tops[u]
        scale = jnp.exp2(top_ref[step] - top)
        total, mixed = None, None
        for n in range(0, listed, 2):
            wa = jnp.exp2(scores[u][:, n * BLK : (n + 1) * BLK] * factor - top)
            wb = jnp.exp2(scores[u][:, (n + 1) * BLK : (n + 2) * BLK] * factor - top)
            total = wa + wb if total is None else total + (wa + wb)
            part = jnp.dot(
                jnp.concatenate([wa.astype(jnp.bfloat16), wb.astype(jnp.bfloat16)], axis=1),
                jnp.concatenate([far[found_s[h, n], 1], far[found_s[h, n + 1], 1]], axis=0),
                preferred_element_type=jnp.float32,
            )
            mixed = part if mixed is None else mixed + part
        total = jnp.sum(total, axis=1, keepdims=True) + total_ref[step] * scale
        mixed = mixed + mixed_ref[step] * scale
        rows = pl.ds(pl.multiple_of(i * BLK, BLK), BLK)
        staged[rows, pl.ds(pl.multiple_of(h * width, width), width)] = (mixed / total).astype(jnp.bfloat16)

    part = heads * width // 2

    def out_refs(k, c):
        i = row_block(k)
        here = staged.at[
            pl.ds(pl.multiple_of(i * BLK, BLK), BLK), pl.ds(pl.multiple_of(c * part, part), part)
        ]
        first = pl.multiple_of((group * 2 + c) * part, part)
        return here, out_ref.at[pl.ds(pl.multiple_of(k // 2 % 2 * BLK, BLK), BLK), pl.ds(first, part)]

    def out_copy(k, c):
        here, there = out_refs(k, c)
        return pltpu.make_async_remote_copy(
            here, there, out_send.at[k * 2 + c], out_recv.at[group * 4 + k // 2 % 2 * 2 + c],
            device_id=owner_of(row_block(k) // 2), device_id_type=MESH,
        )

    def out_keep(k, c):
        here, there = out_refs(k, c)
        return pltpu.make_async_copy(here, there, out_local.at[k // 2 % 2 * 2 + c])

    def kept_here(k):
        return native & (row_block(k) // 2 == head)

    def out_in(of_group, n, c):
        return pltpu.make_async_remote_copy(
            staged.at[pl.ds(0, BLK), pl.ds(0, part)],
            out_ref.at[pl.ds(n * BLK, BLK), pl.ds((of_group * 2 + c) * part, part)],
            out_send.at[0], out_recv.at[of_group * 4 + n * 2 + c],
            device_id=worker_of(jnp.int32(of_group)), device_id_type=MESH,
        )

    def send_part(k, c):
        @pl.when(kept_here(k))
        def _():
            out_keep(k, c).start()

        @pl.when(jnp.logical_not(kept_here(k)))
        def _():
            out_copy(k, c).start()

    def near_steps(k, j, carry):
        first = k * heads + 4 * j
        for u in range(4):
            near_scores(k, 4 * j + u, u)
            near_weigh(lax.rem(first + kept + u - 1, kept), (u + 3) % 4)
            near_mix(lax.rem(first + kept + u - 2, kept), (u + 2) % 4)
        return carry

    def near_group(ks):
        for k in ks:
            lax.fori_loop(0, heads // 4, functools.partial(near_steps, k), 0)
            for name in LATER[k] if k < len(LATER) else []:
                if name == "xp":

                    @pl.when(z == SIDE - 1)
                    def _():
                        event("xp")
                        send(("zpB", -1)).start()

                elif name == "zp":

                    @pl.when(z == 0)
                    def _():
                        event("zp")

                else:
                    event(name)
        last = (ks[-1] + 1) * heads
        near_weigh(jnp.int32(last - 1), 3)
        for u in (2, 3):
            near_mix(jnp.int32(last - 4 + u), u)

    def far_group(ks):
        count, before = len(ks) * heads, ks[0] * heads

        def far_steps(j, carry):
            first = 4 * j
            for u in range(4):
                far_scores(before + lax.rem(first + u + 2, count), (u + 2) % 4)
                far_mix(before + first + u, u)

            send_part(ks[0] + j // 2, j % 2)
            return carry

        for u in range(2):
            far_scores(jnp.int32(before + u), u)
        lax.fori_loop(0, count // 4, far_steps, 0)

    def full_scores(step, u):
        k, h = step // heads, step % heads
        i = row_block(k)
        q = query(late_q, k - EARLY, h)
        own = jnp.dot(q, near[REACH * blocks + i, 0], preferred_element_type=jnp.float32)
        own = jnp.where(causal, own, NEG)
        scores[u][:, :BLK] = own
        top = own
        for n in range(0, 2 * listed, 2):
            if n < listed:
                ref = near
                (a, bias_a), (b, bias_b) = near_entry(i, h, n), near_entry(i, h, n + 1)
            else:
                ref, m = far, n - listed
                a, b = found_s[h, m], found_s[h, m + 1]
                bias_a, bias_b = (far_bias(base + i, h, table_s[1, h, m + d]) for d in range(2))
            sa, sb = pair_scores(q, ref, a, b, bias_a, bias_b)
            scores[u][:, (n + 1) * BLK : (n + 2) * BLK] = sa
            scores[u][:, (n + 2) * BLK : (n + 3) * BLK] = sb
            top = jnp.maximum(top, jnp.maximum(sa, sb))
        tops[u] = jnp.broadcast_to(jnp.max(top, axis=1, keepdims=True) * factor, (BLK, width))

    def full_mix(step, u):
        i, h = row_block(step // heads), step % heads
        top = tops[u]

        def weight(n):
            return jnp.exp2(scores[u][:, n * BLK : (n + 1) * BLK] * factor - top)

        total = weight(0)
        mixed = jnp.dot(
            total.astype(jnp.bfloat16), near[REACH * blocks + i, 1], preferred_element_type=jnp.float32
        )
        for n in range(0, 2 * listed, 2):
            if n < listed:
                ref, a, b = near, near_entry(i, h, n)[0], near_entry(i, h, n + 1)[0]
            else:
                ref, a, b = far, found_s[h, n - listed], found_s[h, n - listed + 1]
            wa, wb = weight(n + 1), weight(n + 2)
            total = total + (wa + wb)
            mixed = mixed + jnp.dot(
                jnp.concatenate([wa.astype(jnp.bfloat16), wb.astype(jnp.bfloat16)], axis=1),
                jnp.concatenate([ref[a, 1], ref[b, 1]], axis=0),
                preferred_element_type=jnp.float32,
            )
        total = jnp.sum(total, axis=1, keepdims=True)
        rows = pl.ds(pl.multiple_of(i * BLK, BLK), BLK)
        staged[rows, pl.ds(pl.multiple_of(h * width, width), width)] = (mixed / total).astype(jnp.bfloat16)

    def full_group(ks):
        count, before = len(ks) * heads, ks[0] * heads

        def full_steps(j, carry):
            first = 4 * j
            for u in range(4):
                full_scores(before + lax.rem(first + u + 2, count), (u + 2) % 4)
                full_mix(before + first + u, u)
            send_part(ks[0] + j // 2, j % 2)
            return carry

        for u in range(2):
            full_scores(jnp.int32(before + u), u)
        lax.fori_loop(0, count // 4, full_steps, 0)

    for k in range(EARLY):
        wait_input(first_query + k)
    near_group(range(EARLY))
    for name in NAMES:
        share(name, 1 - core).wait_recv()
    share("own", 1 - core).wait_recv()
    far_group(range(EARLY))
    for k in range(EARLY, blocks):
        wait_input(first_query + k)
    full_group(range(EARLY, blocks))

    @pl.when(jnp.logical_not(native))
    def _():
        for k in range(len(sources)):
            swap(k).wait_send()

    for c in range(2):
        hop_one(c).wait_send()
        twin_one(c, True).wait_send()
        twin_two(c, True).wait_send()
    hop_two(1).wait_send()

    @pl.when(core == 1)
    def _():
        hop_two(0).wait_send()

    for name in NAMES:
        share(name, core).wait_send()
        if name != "zp":
            send(name).wait_send()

    @pl.when(z == SIDE - 1)
    def _():
        send("zp").wait_send()

    share("own", core).wait_send()

    for k in range(blocks):

        @pl.when(kept_here(k))
        def _():
            for c in range(2):
                out_keep(k, c).wait()

        @pl.when(jnp.logical_not(kept_here(k)))
        def _():
            for c in range(2):
                out_copy(k, c).wait_send()

    for of_group in range(4):

        @pl.when(jnp.logical_not(native & (group == of_group)))
        def _():
            for n in range(2):
                for c in range(2):
                    out_in(of_group, n, c).wait_recv()


def shards(queries, keys, values, vertical, slash):
    width = keys.shape[1]
    rows = queries.shape[0]
    blocks = rows // BLK
    heads, listed = vertical.shape
    groups = lax.axis_size("head")
    k = keys.reshape(blocks, BLK, width)
    v = values.reshape(blocks, BLK, width)
    dma = pltpu.SemaphoreType.DMA
    anywhere = pl.BlockSpec(memory_space=pl.ANY)
    bf16, f32 = jnp.bfloat16, jnp.float32
    inputs = 6 + blocks
    full_width = (2 * listed + 1) * BLK
    return pl.pallas_call(
        functools.partial(layer_kernel, blocks=blocks, heads=heads, width=width, listed=listed),
        in_specs=[anywhere] * 5,
        out_specs=anywhere,
        out_shape=jax.ShapeDtypeStruct((rows // groups, groups * heads * width), bf16),
        scratch_shapes=[
            pltpu.VMEM((2, heads, listed), jnp.int32),
            pltpu.SMEM((2, heads, listed), jnp.int32),
            pltpu.VMEM((heads, listed), jnp.int32),
            pltpu.SMEM((heads, listed), jnp.int32),
            pltpu.SMEM((2, CAP), jnp.int32),
            pltpu.VMEM((EARLY * BLK, heads * width), bf16),
            pltpu.VMEM((rows - EARLY * BLK, heads * width), bf16),
            pltpu.VMEM((blocks, BLK, width), bf16),
            pltpu.VMEM((blocks, 2, BLK, width), bf16),
            pltpu.VMEM((blocks, 2, BLK, width), bf16),
            pltpu.VMEM(((REACH + 1) * blocks, 2, BLK, width), bf16),
            pltpu.VMEM((2 * NODES * CAP, 2, BLK, width), bf16),
            pltpu.VMEM(queries.shape, bf16),
            pltpu.VMEM((heads * EARLY, BLK, width), f32),
            pltpu.VMEM((heads * EARLY, BLK, width), f32),
            pltpu.VMEM((heads * EARLY, BLK, width), f32),
            pltpu.VMEM((BLK, full_width), f32),
            pltpu.VMEM((BLK, full_width), f32),
            pltpu.VMEM((BLK, full_width), f32),
            pltpu.VMEM((BLK, full_width), f32),
            pltpu.VMEM((BLK, full_width), bf16),
            pltpu.VMEM((BLK, full_width), bf16),
            pltpu.VMEM((BLK, full_width), bf16),
            pltpu.VMEM((BLK, full_width), bf16),
            pltpu.VMEM((4, BLK, width), f32),
            dma((inputs,)),
            dma((inputs,)),
            dma((inputs,)),
            dma((2,)),
            dma((8,)),
            dma((8,)),
            dma((len(NAMES),)),
            dma((len(NAMES),)),
            dma((len(NAMES) + 1,)),
            dma((len(NAMES) + 1,)),
            dma((4,)),
            dma((2 * blocks,)),
            dma((4 * groups,)),
        ],
        compiler_params=pltpu.CompilerParams(
            collective_id=0, has_side_effects=True, vmem_limit_bytes=62 * 1024 * 1024
        ),
    )(slash, vertical, queries, k, v)


def solution(mesh):
    in_specs = (
        P("seq", "head"),
        P("seq", "head"),
        P("seq", "head"),
        P("head", None),
        P("head", None),
    )
    out_specs = P(("seq", "head"), None)
    return jax.shard_map(shards, mesh=mesh, in_specs=in_specs, out_specs=out_specs, check_vma=False)
```
